512 devices in a mesh: job: 2 (over y), ta: 16 (over z), xyz: 8 (over x), src: 2 (over core).
Axes of the slice: x: 8, y: 2, z: 16, core: 2. Of those that a mesh axis runs over, the one named last changes fastest.
The devices are a block of a 8x16x16 slice.
Arguments:
- spinors: float32 [64, 32, 2, 8, 3, 2048], P('src', 'ta', None, 'job', None, 'xyz'), parts along dimension 3, may hold values from -6 to 6
- eigvecs: float32 [32, 256, 2, 3, 2048], P('ta', 'job', None, None, 'xyz'), parts along dimension 1, may hold values from -0.0546875 to 0.0546875
- group_of: int32 [32], replicated, may hold values from 0 to 15, as said below
- source_ids: int32 [64], P('src'), may hold values from 0 to 63, as said below
Outputs:
- perambulator: float32 [32, 2, 8, 64, 128], P('ta', None, 'job', 'src', 'xyz'), parts along dimension 2
The draws below stay inside these ranges and needn't reach their ends.
There are 2 independent parts, one for each index of `job`. The reference program is written for one: setup_inputs(seed, part) draws one part's arguments, and reference() takes and returns one part's arrays. A program takes and returns all parts, laid end to end along the dimension named above; an argument that names none is the same for every part. Nothing has to cross between parts.
Inputs may be any that keep to these rules, and one draw needn't show every extreme that they name: `group_of`: every group number appears exactly 2 times. `source_ids`: the 32 entries held by index i of src are a permutation of i * 32 to (i + 1) * 32 - 1.
All inputs are finite; a program needn't handle non-finite values.
Results may differ from the reference program's by a relative error of at most 0.00007.
Values sent between devices are 32-bit elements; how exact they have to be, the bound alone decides.
A program may use at most 64 MiB of HBM per device.

```python
import jax
import jax.numpy as jnp
from jax import lax

K = 128
TL = 2
NS = 32
NT = 32
SITES = 2048
NSRC = 64


def draw_group_of(key, part):
    scores = jax.random.randint(key, (NT,), 0, 1 << 20) * NT + jnp.arange(NT, dtype=jnp.int32)
    shuffle = jnp.argsort(scores).astype(jnp.int32)
    return (jnp.argsort(shuffle).astype(jnp.int32) // TL).astype(jnp.int32)


def draw_source_ids(key, part):
    scores = jax.random.randint(key, (NSRC,), 0, 1 << 20) * NSRC + jnp.arange(NSRC, dtype=jnp.int32)
    blocks = scores.reshape(NSRC // NS, NS)
    within = jnp.argsort(blocks, axis=1).astype(jnp.int32)
    offsets = (jnp.arange(NSRC // NS, dtype=jnp.int32) * NS)[:, None]
    return (within + offsets).reshape(NSRC).astype(jnp.int32)


def levels(own_key, shape, pieces, least, top_value):
    def one(dim, blocks):
        steps = jax.random.uniform(jax.random.fold_in(jax.random.fold_in(own_key, 6), dim), (blocks,), jnp.float32, least / len(pieces), top_value / len(pieces))
        return jnp.repeat(jnp.exp(steps), shape[dim] // blocks).reshape((-1,) + (1,) * (len(shape) - dim - 1))

    loudness = one(*pieces[0])
    for cut in pieces[1:]:
        loudness = loudness * one(*cut)
    return loudness


def centred(rng, shape, width, most, cuts=(), kind=jnp.bfloat16):
    entries = width * jax.random.normal(rng, shape, jnp.float32)
    if cuts:
        entries = entries * levels(rng, shape, cuts, -0.22, 0.18)
    return jnp.clip(entries, -most, most).astype(kind)


def setup_inputs(seed: int = 0, part: int = 0) -> dict:
    streams_of = jax.random.split(jax.random.key(seed), 5)
    part_splits = jax.random.split(jax.random.fold_in(streams_of[4], part), 5)
    return {
        "spinors": centred(part_splits[0], (NSRC, NT, 2, 4, 3, SITES), 1.0, 6.0, ((0, 2), (1, 16), (5, 8)), jnp.float32),
        "eigvecs": centred(part_splits[1], (NT, K, 2, 3, SITES), (6 * SITES) ** -0.5, 0.0546875, ((0, 16), (4, 8)), jnp.float32),
        "group_of": draw_group_of(jax.random.fold_in(streams_of[4], 71), part),
        "source_ids": draw_source_ids(jax.random.fold_in(streams_of[4], 71), part),
    }


def contract_pair(vectors, spinor):
    vector_real = vectors[:, :, 0]
    vector_imag = vectors[:, :, 1]
    spinor_real = spinor[:, :, 0]
    spinor_imag = spinor[:, :, 1]

    def contract(left_side, right_side):
        return jnp.einsum("tkcx,ntscx->tsnk", left_side, right_side, precision=lax.Precision.HIGHEST)

    real_part = contract(vector_real, spinor_real) + contract(vector_imag, spinor_imag)
    imag_part = contract(vector_real, spinor_imag) - contract(vector_imag, spinor_real)
    return jnp.stack([real_part, imag_part], axis=1)


def reference(spinors, eigvecs, group_of, source_ids):
    extent = group_of.shape[0]
    sort_keys = group_of.astype(jnp.int32) * extent + jnp.arange(extent, dtype=jnp.int32)
    ordering = jnp.argsort(sort_keys).astype(jnp.int32)

    def one_slice(position):
        timeslice = ordering[position]
        vectors = lax.dynamic_slice_in_dim(eigvecs, position, 1, 0)
        spinor = lax.dynamic_slice_in_dim(spinors, timeslice, 1, 1)
        return contract_pair(vectors, spinor)[0]

    projected = lax.map(one_slice, jnp.arange(extent, dtype=jnp.int32))
    inverse = jnp.argsort(source_ids).astype(jnp.int32)
    return jnp.take(projected, inverse, axis=3)
```

```python
import functools

import jax
import jax.numpy as jnp
from jax import lax
from jax.experimental import pallas as pl
from jax.experimental.pallas import tpu as pltpu
from jax.sharding import PartitionSpec as P

MESH = pl.DeviceIdType.MESH
LANES = 128
Q = 2


def kernel(sizes, group_ref, ids_ref, vec_ref, spin_ref, out_ref,
           rank, order, inverse, raw, both, high, low, mids, mail, gathered, left,
           part, parts, home, relay, post, back,
           load_sem, own_sem, pair_sem, s1, r1, s2, r2, s3, r3, s4, r4, s5, r5):
    nz, nx, nc, ns, nt, spin, depth, keep = sizes
    z, x, c = lax.axis_index("ta"), lax.axis_index("xyz"), lax.axis_index("src")
    other = 1 - c
    rows = ns * spin
    chunk = keep * depth
    half = nx // nc

    def far(d):
        return lax.rem(z + d, nz)

    barrier = pltpu.get_barrier_semaphore()

    @pl.loop(1, nz)
    def _(d):
        pl.semaphore_signal(barrier, inc=1, device_id={"ta": far(d)}, device_id_type=MESH)

    @pl.loop(1, nx)
    def _(d):
        there = lax.rem(x + d, nx)
        for core in range(nc):
            pl.semaphore_signal(barrier, inc=1, device_id={"xyz": there, "src": core}, device_id_type=MESH)

    pl.semaphore_signal(barrier, inc=1, device_id={"src": other}, device_id_type=MESH)

    load = pltpu.make_async_copy(spin_ref, raw, load_sem)
    load.start()
    pl.semaphore_wait(barrier, (nz - 1) + (nx - 1) * nc + 1)

    def share(q, there):
        first = (c * (nz * Q * keep) + there * (Q * keep) + q * keep) * depth
        return vec_ref.at[:, pl.ds(pl.multiple_of(first, 8), chunk), :]

    def spread(q, d):
        return pltpu.make_async_remote_copy(
            src_ref=share(q, far(d)), dst_ref=mids[q].at[pl.ds(nt * z, nt)],
            send_sem=s1.at[q, d], recv_sem=r1.at[q, d], device_id={"ta": far(d)}, device_id_type=MESH)

    def deliver(q, d):
        return pltpu.make_async_remote_copy(
            src_ref=mail.at[q, d], dst_ref=gathered.at[q, :, pl.ds(pl.multiple_of(z * chunk, 8), chunk), :],
            send_sem=s2.at[q, d], recv_sem=r2.at[q, d], device_id={"ta": far(d)}, device_id_type=MESH)

    for q in range(Q):
        @pl.loop(1, nz)
        def _(d):
            spread(q, d).start()

        pltpu.make_async_copy(share(q, z), mids[q].at[pl.ds(nt * z, nt)], own_sem.at[q]).start()

    count = nz * nt

    @pl.loop(0, count)
    def _(t):
        mine = group_ref[t] * count + t
        total = jnp.int32(0)
        for u in range(count):
            total += jnp.where(group_ref[u] * count + u < mine, 1, 0)
        rank[t] = total

    @pl.loop(0, count)
    def _(r):
        total = jnp.int32(0)
        for u in range(count):
            total = jnp.maximum(total, jnp.where(rank[u] == r, u, 0))
        order[r] = total

    @pl.loop(0, ns)
    def _(j):
        total = jnp.int32(0)
        for u in range(ns):
            total = jnp.maximum(total, jnp.where(ids_ref[u] - c * ns == j, u, 0))
        inverse[j] = total

    load.wait()

    @pl.loop(0, ns)
    def _(j):
        n = inverse[j]
        for tl in range(nt):
            for g in range(depth):
                for s in range(spin):
                    both[c, tl, g, pl.ds(s * ns + j, 1), :] = raw[n, tl, g * spin + s:g * spin + s + 1, :]

    pair = pltpu.make_async_remote_copy(
        src_ref=both.at[c], dst_ref=both.at[c], send_sem=pair_sem.at[0], recv_sem=pair_sem.at[1],
        device_id={"src": other}, device_id_type=MESH)
    pair.start()
    pair.wait()

    @pl.loop(0, nt)
    def _(tl):
        for core in range(nc):
            for g in range(depth):
                block = both[core, tl, g]
                top = block.astype(jnp.bfloat16)
                high[tl, core * rows:(core + 1) * rows, g * LANES:(g + 1) * LANES] = top
                low[tl, core * rows:(core + 1) * rows, g * LANES:(g + 1) * LANES] = (block - top.astype(jnp.float32)).astype(jnp.bfloat16)

    for q in range(Q):
        @pl.loop(1, nz)
        def _(d):
            spread(q, d).wait_recv()

        pltpu.make_async_copy(share(q, z), mids[q].at[pl.ds(nt * z, nt)], own_sem.at[q]).wait()

        @pl.loop(1, nz)
        def _(d):
            for tl in range(nt):
                mail[q, d, tl] = mids[q][rank[nt * far(d) + tl]]

        for tl in range(nt):
            gathered[q, tl, pl.ds(pl.multiple_of(z * chunk, 8), chunk), :] = mids[q][rank[nt * z + tl]]

        @pl.loop(1, nz)
        def _(d):
            deliver(q, d).start()

    contract = (((1,), (1,)), ((), ()))
    ks = nz * keep
    colours = depth // 4

    def reduce_copy(q, xs, core):
        return pltpu.make_async_remote_copy(
            src_ref=part.at[q, xs, core], dst_ref=parts.at[q, x],
            send_sem=s3.at[q, xs, core], recv_sem=r3.at[q, x],
            device_id={"xyz": half * c + xs, "src": core}, device_id_type=MESH)

    sender = lax.div(x, half)
    for q in range(Q):
        @pl.loop(1, nz)
        def _(d):
            deliver(q, d).wait_recv()

        for tl in range(nt):
            for i in range(colours):
                for b in range(2):
                    re = gathered[q, tl, pl.ds(i * 4 + b * 2, ks, stride=depth), :]
                    im = gathered[q, tl, pl.ds(i * 4 + b * 2 + 1, ks, stride=depth), :]
                    g = i * 2 + b
                    for at, value in ((0, re), (depth // 2, im)):
                        top = value.astype(jnp.bfloat16)
                        rest = (value - top.astype(jnp.float32)).astype(jnp.bfloat16)
                        where = slice((at + g) * LANES, (at + g + 1) * LANES)
                        cross = slice((depth // 2 - at + g) * LANES, (depth // 2 - at + g + 1) * LANES)
                        left[0:ks, where] = top
                        left[2 * ks:3 * ks, where] = rest
                        left[ks:2 * ks, cross] = top if at == 0 else -top
                        left[3 * ks:4 * ks, cross] = rest if at == 0 else -rest
            one = lax.dot_general(left[...], high[tl], contract, preferred_element_type=jnp.float32)
            two = lax.dot_general(left[0:2 * ks, :], low[tl], contract, preferred_element_type=jnp.float32)
            total = one[0:2 * ks] + one[2 * ks:4 * ks] + two
            step = ks // half
            for xs in range(half):
                for core in range(nc):
                    for reim in range(2):
                        part[q, xs, core, tl, reim] = total[reim * ks + xs * step:reim * ks + (xs + 1) * step, core * rows:(core + 1) * rows]

        for xs in range(half):
            for core in range(nc):
                mine = jnp.logical_and(half * c + xs == x, c == core)

                @pl.when(jnp.logical_not(mine))
                def _():
                    reduce_copy(q, xs, core).start()

                @pl.when(mine)
                def _():
                    parts[q, x] = part[q, xs, core]

    def return_copy(d):
        return pltpu.make_async_remote_copy(
            src_ref=home.at[far(d)], dst_ref=relay.at[pl.ds(nt * z, nt)],
            send_sem=s4.at[d], recv_sem=r4.at[d], device_id={"ta": far(d)}, device_id_type=MESH)

    def final_copy(d):
        return pltpu.make_async_remote_copy(
            src_ref=post.at[far(d)], dst_ref=back.at[z],
            send_sem=s5.at[d], recv_sem=r5.at[d], device_id={"ta": far(d)}, device_id_type=MESH)

    per = nz // (Q * 2)
    for q in range(Q):
        for xs in range(nx):
            @pl.when(jnp.logical_not(jnp.logical_and(xs == x, sender == c)))
            def _():
                pltpu.make_async_remote_copy(
                    src_ref=part.at[q, 0, 0], dst_ref=parts.at[q, xs], send_sem=s3.at[q, 0, 0], recv_sem=r3.at[q, xs],
                    device_id={"src": other}, device_id_type=MESH).wait_recv()

        for tl in range(nt):
            for reim in range(2):
                total = parts[q, 0, tl, reim]
                for xs in range(1, nx):
                    total += parts[q, xs, tl, reim]
                for i in range(per):
                    home[(q * 2 + reim) * per + i, tl] = total[i * keep:(i + 1) * keep, :]

    @pl.loop(1, nz)
    def _(d):
        return_copy(d).start()

    for tl in range(nt):
        relay[nt * z + tl] = home[z, tl]

    @pl.loop(1, nz)
    def _(d):
        return_copy(d).wait_recv()

    @pl.loop(0, nz)
    def _(there):
        for tl in range(nt):
            post[there, tl] = relay[order[nt * there + tl]]

    @pl.loop(1, nz)
    def _(d):
        final_copy(d).start()

    back[z] = post[z]

    @pl.loop(1, nz)
    def _(d):
        final_copy(d).wait_recv()

    for q in range(Q):
        for reim in range(2):
            for i in range(per):
                for tl in range(nt):
                    at = i * Q * keep + q * keep
                    out_ref[tl, reim, at:at + keep, :] = back[(q * 2 + reim) * per + i, tl]

    for q in range(Q):
        @pl.loop(1, nz)
        def _(d):
            spread(q, d).wait_send()
            deliver(q, d).wait_send()

        for xs in range(half):
            for core in range(nc):
                @pl.when(jnp.logical_not(jnp.logical_and(half * c + xs == x, c == core)))
                def _():
                    reduce_copy(q, xs, core).wait_send()

    @pl.loop(1, nz)
    def _(d):
        return_copy(d).wait_send()
        final_copy(d).wait_send()


def solution(mesh):
    nz, nx, nc = mesh.shape["ta"], mesh.shape["xyz"], mesh.shape["src"]

    def local(spinors, eigvecs, group_of, source_ids):
        ns, nt, _, spin, colours, sites = spinors.shape
        kk = eigvecs.shape[1]
        blocks = sites // LANES
        depth = 2 * colours * blocks
        keep = kk // (nc * nz * Q)
        rows = ns * spin
        ks = nz * keep
        spin_view = spinors.transpose(0, 1, 2, 4, 3, 5).reshape(ns, nt, 2, colours, spin, blocks, LANES)
        spin_view = spin_view.transpose(0, 1, 2, 3, 5, 4, 6).reshape(ns, nt, depth * spin, LANES)
        vec_view = eigvecs.transpose(0, 1, 3, 2, 4).reshape(nt, kk, colours, 2, blocks, LANES)
        vec_view = vec_view.transpose(0, 1, 2, 4, 3, 5).reshape(nt, kk * depth, LANES)
        sizes = (nz, nx, nc, ns, nt, spin, depth, keep)
        f32, bf16 = jnp.float32, jnp.bfloat16
        dma = pltpu.SemaphoreType.DMA
        small = (keep, LANES)
        flat = pl.pallas_call(
            functools.partial(kernel, sizes),
            out_shape=jax.ShapeDtypeStruct((nt, 2, kk // nx, rows), f32),
            in_specs=[pl.BlockSpec(memory_space=pltpu.SMEM)] * 2 + [pl.BlockSpec(memory_space=pl.ANY)] * 2,
            out_specs=pl.BlockSpec(memory_space=pltpu.VMEM),
            scratch_shapes=[
                pltpu.SMEM((nz * nt,), jnp.int32),
                pltpu.SMEM((nz * nt,), jnp.int32),
                pltpu.SMEM((ns,), jnp.int32),
                pltpu.VMEM((ns, nt, depth * spin, LANES), f32),
                pltpu.VMEM((nc, nt, depth, rows, LANES), f32),
                pltpu.VMEM((nt, nc * rows, depth * LANES), bf16),
                pltpu.VMEM((nt, nc * rows, depth * LANES), bf16),
                [pltpu.VMEM((nz * nt, keep * depth, LANES), f32)] * Q,
                pltpu.VMEM((Q, nz, nt, keep * depth, LANES), f32),
                pltpu.VMEM((Q, nt, ks * depth, LANES), f32),
                pltpu.VMEM((4 * ks, depth * LANES), bf16),
                pltpu.VMEM((Q, nx // nc, nc, nt, 2, ks * nc // nx, LANES), f32),
                pltpu.VMEM((Q, nx, nt, 2, ks * nc // nx, LANES), f32),
                pltpu.VMEM((nz, nt) + small, f32),
                pltpu.VMEM((nz * nt,) + small, f32),
                pltpu.VMEM((nz, nt) + small, f32),
                pltpu.VMEM((nz, nt) + small, f32),
                dma, dma((Q,)), dma((2,)),
                dma((Q, nz)), dma((Q, nz)), dma((Q, nz)), dma((Q, nz)),
                dma((Q, nx // nc, nc)), dma((Q, nx)),
                dma((nz,)), dma((nz,)), dma((nz,)), dma((nz,)),
            ],
            compiler_params=pltpu.CompilerParams(collective_id=0, has_side_effects=True),
        )(group_of, source_ids, vec_view, spin_view)
        return flat.reshape(nt, 2, kk // nx, spin, ns).transpose(0, 1, 3, 4, 2)

    in_specs = (
        P("src", "ta", None, "job", None, "xyz"),
        P("ta", "job", None, None, "xyz"),
        P(),
        P("src"),
    )
    out_specs = P("ta", None, "job", "src", "xyz")
    return jax.shard_map(local, mesh=mesh, in_specs=in_specs, out_specs=out_specs, check_vma=False)
```

```python
import functools

import jax
import jax.numpy as jnp
from jax import lax
from jax.experimental import pallas as pl
from jax.experimental.pallas import tpu as pltpu
from jax.sharding import PartitionSpec as P

MESH = pl.DeviceIdType.MESH
LANES = 128
Q = 2


def kernel(sizes, group_ref, ids_ref, vec_ref, spin_ref, out_ref,
           rank, order, inverse, raw, both, high, low, mids, mail, gathered, left,
           part, parts, home, relay, post, back, flat,
           load_sem, own_sem, pair_sem, s1, r1, s2, r2, s3, r3, s4, r4, s5, r5):
    nz, nx, nc, ns, nt, spin, depth, keep = sizes
    z, x, c = lax.axis_index("ta"), lax.axis_index("xyz"), lax.axis_index("src")
    other = 1 - c
    rows = ns * spin
    chunk = keep * depth
    half = nx // nc

    def far(d):
        return lax.rem(z + d, nz)

    barrier = pltpu.get_barrier_semaphore()

    @pl.loop(1, nz)
    def _(d):
        pl.semaphore_signal(barrier, inc=1, device_id={"ta": far(d)}, device_id_type=MESH)

    @pl.loop(1, nx)
    def _(d):
        there = lax.rem(x + d, nx)
        for core in range(nc):
            pl.semaphore_signal(barrier, inc=1, device_id={"xyz": there, "src": core}, device_id_type=MESH)

    pl.semaphore_signal(barrier, inc=1, device_id={"src": other}, device_id_type=MESH)

    load = pltpu.make_async_copy(spin_ref, raw, load_sem)
    load.start()
    pl.semaphore_wait(barrier, (nz - 1) + (nx - 1) * nc + 1)

    def share(q, there):
        first = (c * (nz * Q * keep) + there * (Q * keep) + q * keep) * depth
        return vec_ref.at[:, pl.ds(pl.multiple_of(first, 8), chunk), :]

    def spread(q, d):
        return pltpu.make_async_remote_copy(
            src_ref=share(q, far(d)), dst_ref=mids[q].at[pl.ds(nt * z, nt)],
            send_sem=s1.at[q, d], recv_sem=r1.at[q, d], device_id={"ta": far(d)}, device_id_type=MESH)

    def deliver(q, d):
        return pltpu.make_async_remote_copy(
            src_ref=mail.at[q, d], dst_ref=gathered.at[q, :, pl.ds(pl.multiple_of(z * chunk, 8), chunk), :],
            send_sem=s2.at[q, d], recv_sem=r2.at[q, d], device_id={"ta": far(d)}, device_id_type=MESH)

    outward = sorted(range(1, nz), key=lambda d: -min(d, nz - d))
    for q in range(Q):
        for d in outward:
            spread(q, d).start()

        pltpu.make_async_copy(share(q, z), mids[q].at[pl.ds(nt * z, nt)], own_sem.at[q]).start()

    count = nz * nt

    @pl.loop(0, count)
    def _(t):
        mine = group_ref[t] * count + t
        total = jnp.int32(0)
        for u in range(count):
            total += jnp.where(group_ref[u] * count + u < mine, 1, 0)
        rank[t] = total

    @pl.loop(0, count)
    def _(r):
        total = jnp.int32(0)
        for u in range(count):
            total = jnp.maximum(total, jnp.where(rank[u] == r, u, 0))
        order[r] = total

    @pl.loop(0, ns)
    def _(j):
        total = jnp.int32(0)
        for u in range(ns):
            total = jnp.maximum(total, jnp.where(ids_ref[u] - c * ns == j, u, 0))
        inverse[j] = total

    load.wait()

    @pl.loop(0, ns)
    def _(j):
        n = inverse[j]
        for tl in range(nt):
            for g in range(depth):
                for s in range(spin):
                    both[c, tl, g, pl.ds(s * ns + j, 1), :] = raw[n, tl, g * spin + s:g * spin + s + 1, :]

    pair = pltpu.make_async_remote_copy(
        src_ref=both.at[c], dst_ref=both.at[c], send_sem=pair_sem.at[0], recv_sem=pair_sem.at[1],
        device_id={"src": other}, device_id_type=MESH)
    pair.start()
    pair.wait()

    @pl.loop(0, nt)
    def _(tl):
        for core in range(nc):
            for g in range(depth):
                block = both[core, tl, g]
                top = block.astype(jnp.bfloat16)
                high[tl, core * rows:(core + 1) * rows, g * LANES:(g + 1) * LANES] = top
                low[tl, core * rows:(core + 1) * rows, g * LANES:(g + 1) * LANES] = (block - top.astype(jnp.float32)).astype(jnp.bfloat16)

    for q in range(Q):
        with jax.named_scope("mid%d" % q):
            @pl.loop(1, nz)
            def _(d):
                spread(q, d).wait_recv()

        pltpu.make_async_copy(share(q, z), mids[q].at[pl.ds(nt * z, nt)], own_sem.at[q]).wait()

        @pl.loop(1, nz)
        def _(d):
            for tl in range(nt):
                mail[q, d, tl] = mids[q][rank[nt * far(d) + tl]]

        for tl in range(nt):
            gathered[q, tl, pl.ds(pl.multiple_of(z * chunk, 8), chunk), :] = mids[q][rank[nt * z + tl]]

        for d in outward:
            deliver(q, d).start()

    contract = (((1,), (1,)), ((), ()))
    ks = nz * keep
    colours = depth // 4

    def reduce_copy(q, xs, core):
        return pltpu.make_async_remote_copy(
            src_ref=part.at[q, xs, core], dst_ref=parts.at[q, x],
            send_sem=s3.at[q, xs, core], recv_sem=r3.at[q, x],
            device_id={"xyz": half * c + xs, "src": core}, device_id_type=MESH)

    sender = lax.div(x, half)
    per = nz // (Q * 2)
    relays = 2 * per
    step = ks // half

    def relay_at(i):
        return lax.rem(i + nz - relays // 4, nz)

    my_relay = lax.rem(z + relays // 4, nz)

    def contract_chunk(q):
        with jax.named_scope("got%d" % q):
            @pl.loop(1, nz)
            def _(d):
                deliver(q, d).wait_recv()

        for tl in range(nt):
            for i in range(colours):
                for b in range(2):
                    re = gathered[q, tl, pl.ds(i * 4 + b * 2, ks, stride=depth), :]
                    im = gathered[q, tl, pl.ds(i * 4 + b * 2 + 1, ks, stride=depth), :]
                    g = i * 2 + b
                    for at, value in ((0, re), (depth // 2, im)):
                        top = value.astype(jnp.bfloat16)
                        rest = (value - top.astype(jnp.float32)).astype(jnp.bfloat16)
                        where = slice((at + g) * LANES, (at + g + 1) * LANES)
                        cross = slice((depth // 2 - at + g) * LANES, (depth // 2 - at + g + 1) * LANES)
                        left[0:ks, where] = top
                        left[2 * ks:3 * ks, where] = rest
                        left[ks:2 * ks, cross] = top if at == 0 else -top
                        left[3 * ks:4 * ks, cross] = rest if at == 0 else -rest
            one = lax.dot_general(left[...], high[tl], contract, preferred_element_type=jnp.float32)
            two = lax.dot_general(left[0:2 * ks, :], low[tl], contract, preferred_element_type=jnp.float32)
            total = one[0:2 * ks] + one[2 * ks:4 * ks] + two
            for xs in range(half):
                for core in range(nc):
                    for reim in range(2):
                        part[q, xs, core, tl, reim] = total[reim * ks + xs * step:reim * ks + (xs + 1) * step, core * rows:(core + 1) * rows]

        for xs in range(half):
            for core in range(nc):
                mine = jnp.logical_and(half * c + xs == x, c == core)

                @pl.when(jnp.logical_not(mine))
                def _():
                    reduce_copy(q, xs, core).start()

                @pl.when(mine)
                def _():
                    parts[q, x] = part[q, xs, core]

    def return_copy(q, i):
        return pltpu.make_async_remote_copy(
            src_ref=home.at[q, i], dst_ref=relay[q].at[pl.ds(nt * z, nt)],
            send_sem=s4.at[q, i], recv_sem=r4.at[q, z], device_id={"ta": relay_at(i)}, device_id_type=MESH)

    def arrival(q, there):
        return pltpu.make_async_remote_copy(
            src_ref=home.at[q, 0], dst_ref=relay[q].at[pl.ds(nt * there, nt)],
            send_sem=s4.at[q, 0], recv_sem=r4.at[q, there], device_id={"src": other}, device_id_type=MESH)

    def final_copy(q, d):
        return pltpu.make_async_remote_copy(
            src_ref=post.at[q, far(d)], dst_ref=back.at[q, my_relay],
            send_sem=s5.at[q, d], recv_sem=r5.at[q, my_relay], device_id={"ta": far(d)}, device_id_type=MESH)

    def final_arrival(q, i):
        return pltpu.make_async_remote_copy(
            src_ref=post.at[q, 0], dst_ref=back.at[q, i],
            send_sem=s5.at[q, 0], recv_sem=r5.at[q, i], device_id={"src": other}, device_id_type=MESH)

    def reduce_chunk(q):
        with jax.named_scope("reduced%d" % q):
            for xs in range(nx):
                @pl.when(jnp.logical_not(jnp.logical_and(xs == x, sender == c)))
                def _():
                    pltpu.make_async_remote_copy(
                        src_ref=part.at[q, 0, 0], dst_ref=parts.at[q, xs], send_sem=s3.at[q, 0, 0], recv_sem=r3.at[q, xs],
                        device_id={"src": other}, device_id_type=MESH).wait_recv()

        for tl in range(nt):
            for reim in range(2):
                total = parts[q, 0, tl, reim]
                for xs in range(1, nx):
                    total += parts[q, xs, tl, reim]
                for i in range(per):
                    home[q, reim * per + i, tl] = total[i * keep:(i + 1) * keep, :]

        for i in range(relays):
            @pl.when(relay_at(i) != z)
            def _():
                return_copy(q, i).start()

            @pl.when(relay_at(i) == z)
            def _():
                for tl in range(nt):
                    relay[q][nt * z + tl] = home[q, i, tl]

    def relay_chunk(q):
        @pl.when(my_relay < relays)
        def _():
            with jax.named_scope("relayed%d" % q):
                @pl.loop(0, nz)
                def _(there):
                    @pl.when(there != z)
                    def _():
                        arrival(q, there).wait_recv()

            @pl.loop(0, nz)
            def _(there):
                for tl in range(nt):
                    post[q, there, tl] = relay[q][order[nt * there + tl]]

            for d in range(1, nz):
                final_copy(q, d).start()

            back[q, my_relay] = post[q, z]

    contract_chunk(0)
    for q in range(Q):
        reduce_chunk(q)
        if q + 1 < Q:
            contract_chunk(q + 1)
            relay_chunk(q)
    relay_chunk(Q - 1)

    for q in range(Q):
        @pl.loop(1, nz)
        def _(d):
            spread(q, d).wait_send()
            deliver(q, d).wait_send()

        for xs in range(half):
            for core in range(nc):
                @pl.when(jnp.logical_not(jnp.logical_and(half * c + xs == x, c == core)))
                def _():
                    reduce_copy(q, xs, core).wait_send()

        for i in range(relays):
            @pl.when(relay_at(i) != z)
            def _():
                return_copy(q, i).wait_send()

    for q in range(Q):
        with jax.named_scope("final%d" % q):
            @pl.loop(0, relays)
            def _(i):
                @pl.when(i != my_relay)
                def _():
                    final_arrival(q, i).wait_recv()

        for reim in range(2):
            for i in range(per):
                for tl in range(nt):
                    at = i * Q * keep + q * keep
                    flat[tl, reim, at:at + keep, :] = back[q, reim * per + i, tl]

    for s in range(spin):
        out_ref[:, :, s] = flat[:, :, :, s * ns:(s + 1) * ns]

    @pl.when(my_relay < relays)
    def _():
        for q in range(Q):
            @pl.loop(1, nz)
            def _(d):
                final_copy(q, d).wait_send()


def solution(mesh):
    nz, nx, nc = mesh.shape["ta"], mesh.shape["xyz"], mesh.shape["src"]

    def local(spinors, eigvecs, group_of, source_ids):
        ns, nt, _, spin, colours, sites = spinors.shape
        kk = eigvecs.shape[1]
        blocks = sites // LANES
        depth = 2 * colours * blocks
        keep = kk // (nc * nz * Q)
        rows = ns * spin
        ks = nz * keep
        spin_view = spinors.transpose(0, 1, 2, 4, 3, 5).reshape(ns, nt, 2, colours, spin, blocks, LANES)
        spin_view = spin_view.transpose(0, 1, 2, 3, 5, 4, 6).reshape(ns, nt, depth * spin, LANES)
        vec_view = eigvecs.transpose(0, 1, 3, 2, 4).reshape(nt, kk, colours, 2, blocks, LANES)
        vec_view = vec_view.transpose(0, 1, 2, 4, 3, 5).reshape(nt, kk * depth, LANES)
        sizes = (nz, nx, nc, ns, nt, spin, depth, keep)
        f32, bf16 = jnp.float32, jnp.bfloat16
        dma = pltpu.SemaphoreType.DMA
        small = (keep, LANES)
        out = pl.pallas_call(
            functools.partial(kernel, sizes),
            out_shape=jax.ShapeDtypeStruct((nt, 2, spin, kk // nx, ns), f32),
            in_specs=[pl.BlockSpec(memory_space=pltpu.SMEM)] * 2 + [pl.BlockSpec(memory_space=pl.ANY)] * 2,
            out_specs=pl.BlockSpec(memory_space=pltpu.VMEM),
            scratch_shapes=[
                pltpu.SMEM((nz * nt,), jnp.int32),
                pltpu.SMEM((nz * nt,), jnp.int32),
                pltpu.SMEM((ns,), jnp.int32),
                pltpu.VMEM((ns, nt, depth * spin, LANES), f32),
                pltpu.VMEM((nc, nt, depth, rows, LANES), f32),
                pltpu.VMEM((nt, nc * rows, depth * LANES), bf16),
                pltpu.VMEM((nt, nc * rows, depth * LANES), bf16),
                [pltpu.VMEM((nz * nt, keep * depth, LANES), f32)] * Q,
                pltpu.VMEM((Q, nz, nt, keep * depth, LANES), f32),
                pltpu.VMEM((Q, nt, ks * depth, LANES), f32),
                pltpu.VMEM((4 * ks, depth * LANES), bf16),
                pltpu.VMEM((Q, nx // nc, nc, nt, 2, ks * nc // nx, LANES), f32),
                pltpu.VMEM((Q, nx, nt, 2, ks * nc // nx, LANES), f32),
                pltpu.VMEM((Q, nz // Q, nt) + small, f32),
                [pltpu.VMEM((nz * nt,) + small, f32)] * Q,
                pltpu.VMEM((Q, nz, nt) + small, f32),
                pltpu.VMEM((Q, nz // Q, nt) + small, f32),
                pltpu.VMEM((nt, 2, kk // nx, rows), f32),
                dma, dma((Q,)), dma((2,)),
                dma((Q, nz)), dma((Q, nz)), dma((Q, nz)), dma((Q, nz)),
                dma((Q, nx // nc, nc)), dma((Q, nx)),
                dma((Q, nz // Q)), dma((Q, nz)), dma((Q, nz)), dma((Q, nz // Q)),
            ],
            compiler_params=pltpu.CompilerParams(collective_id=0, has_side_effects=True),
        )(group_of, source_ids, vec_view, spin_view)
        return out.transpose(0, 1, 2, 4, 3)

    in_specs = (
        P("src", "ta", None, "job", None, "xyz"),
        P("ta", "job", None, None, "xyz"),
        P(),
        P("src"),
    )
    out_specs = P("ta", None, "job", "src", "xyz")
    return jax.shard_map(local, mesh=mesh, in_specs=in_specs, out_specs=out_specs, check_vma=False)
```

```python
import functools

import jax
import jax.numpy as jnp
from jax import lax
from jax.experimental import pallas as pl
from jax.experimental.pallas import tpu as pltpu
from jax.sharding import PartitionSpec as P

MESH = pl.DeviceIdType.MESH
LANES = 128
Q = 2
EARLY = 12
LATE = 0
RELAYS = 4
BEFORE = 1


def kernel(sizes, group_hbm, ids_hbm, vec_ref, spin_ref, out_ref,
           group_ref, ids_ref, rank, order, inverse, raw, both, high, low, mids, mail, gathered, left,
           part, parts, home, relay, post, back, flat,
           above, along, small_sem, load_sem, own_sem, pair_sem, *pairs):
    (s1, r1), (s2, r2), (s3, r3), (s4, r4), (s5, r5) = pairs
    nz, nx, nc, ns, nt, spin, depth, keep, relays = sizes
    z, x, c = lax.axis_index("ta"), lax.axis_index("xyz"), lax.axis_index("src")
    other = 1 - c
    rows = ns * spin
    chunk = keep * depth
    half = nx // nc

    def far(d):
        return lax.rem(z + d, nz)

    def settle(ref, sem):
        pltpu.make_async_copy(ref, ref, sem).wait()

    place = lax.rem(z + nz - 1, nz)

    def at_place(p):
        return lax.rem(p + 1, nz)

    barrier = pltpu.get_barrier_semaphore()

    @pl.loop(0, nz - 1 - place)
    def _(i):
        pl.semaphore_signal(barrier, inc=1, device_id={"ta": at_place(nz - 1 - i)}, device_id_type=MESH)

    right, left_x = lax.rem(x + 1, nx), lax.rem(x + nx - 1, nx)
    for there in (right, left_x):
        pl.semaphore_signal(barrier, inc=1, device_id={"xyz": there}, device_id_type=MESH)
    pl.semaphore_signal(barrier, inc=1, device_id={"src": other}, device_id_type=MESH)

    loads = [
        pltpu.make_async_copy(group_hbm, group_ref, small_sem.at[0]),
        pltpu.make_async_copy(ids_hbm, ids_ref, small_sem.at[1]),
        pltpu.make_async_copy(spin_ref, raw, load_sem),
    ]
    for load in loads:
        load.start()
    pl.semaphore_wait(barrier, 3 + place)

    def share(q, there):
        first = (c * (nz * Q * keep) + there * (Q * keep) + q * keep) * depth
        return vec_ref.at[:, pl.ds(pl.multiple_of(first, 8), chunk), :]

    def spread(q, d):
        return pltpu.make_async_remote_copy(
            src_ref=share(q, far(d)), dst_ref=mids[q].at[pl.ds(nt * z, nt)],
            send_sem=s1.at[q], recv_sem=r1.at[q], device_id={"ta": far(d)}, device_id_type=MESH)

    def deliver(q, d):
        return pltpu.make_async_remote_copy(
            src_ref=mail.at[q, d], dst_ref=gathered.at[q, :, pl.ds(pl.multiple_of(z * chunk, 8), chunk), :],
            send_sem=s2.at[q], recv_sem=r2.at[q], device_id={"ta": far(d)}, device_id_type=MESH)

    outward = sorted(range(1, nz), key=lambda d: -min(d, nz - d))
    with jax.named_scope("known"):
      for d in outward:
        @pl.when(d >= nz - place)
        def _():
            pl.semaphore_signal(above.at[place], inc=1, device_id={"ta": far(d)}, device_id_type=MESH)

    for q in range(Q):
        for d in outward:
            @pl.when(d >= nz - place)
            def _():
                spread(q, d).start()

        pltpu.make_async_copy(share(q, z), mids[q].at[pl.ds(nt * z, nt)], own_sem.at[q]).start()

    count = nz * nt

    def prepare():
        hops = list(range(nx // 2 - 1))

        def tell(j):
            pl.semaphore_signal(along.at[0, j], inc=1, device_id={"xyz": left_x}, device_id_type=MESH)
            pl.semaphore_signal(along.at[1, j], inc=1, device_id={"xyz": right}, device_id_type=MESH)

        def hear(j):
            pl.semaphore_wait(along.at[0, j], 1)
            pl.semaphore_wait(along.at[1, j], 1)

        tell(hops[0])
        loads[0].wait()
        loads[1].wait()


        @pl.loop(0, count)
        def _(t):
            mine = group_ref[t] * count + t
            total = jnp.int32(0)
            for u in range(count):
                total += jnp.where(group_ref[u] * count + u < mine, 1, 0)
            rank[t] = total

        @pl.loop(0, count)
        def _(r):
            total = jnp.int32(0)
            for u in range(count):
                total = jnp.maximum(total, jnp.where(rank[u] == r, u, 0))
            order[r] = total

        @pl.loop(0, ns)
        def _(j):
            total = jnp.int32(0)
            for u in range(ns):
                total = jnp.maximum(total, jnp.where(ids_ref[u] - c * ns == j, u, 0))
            inverse[j] = total

        for j in hops[:-1]:
            hear(j)
            tell(j + 1)
        loads[2].wait()

        @pl.loop(0, ns)
        def _(j):
            n = inverse[j]
            for tl in range(nt):
                for g in range(depth):
                    for s in range(spin):
                        both[c, tl, g, pl.ds(s * ns + j, 1), :] = raw[n, tl, g * spin + s:g * spin + s + 1, :]

        pair = pltpu.make_async_remote_copy(
            src_ref=both.at[c], dst_ref=both.at[c], send_sem=pair_sem.at[0], recv_sem=pair_sem.at[1],
            device_id={"src": other}, device_id_type=MESH)
        hear(hops[-1])
        pair.start()
        pair.wait()

        @pl.loop(0, nt)
        def _(tl):
            for core in range(nc):
                for g in range(depth):
                    block = both[core, tl, g]
                    top = block.astype(jnp.bfloat16)
                    high[tl, core * rows:(core + 1) * rows, g * LANES:(g + 1) * LANES] = top
                    low[tl, core * rows:(core + 1) * rows, g * LANES:(g + 1) * LANES] = (block - top.astype(jnp.float32)).astype(jnp.bfloat16)

    with jax.named_scope("early"):
        @pl.when(place < EARLY)
        def _():
            prepare()

    with jax.named_scope("upper"):
        @pl.loop(1, jnp.maximum(LATE - place, 1))
        def _(d):
            pl.semaphore_wait(above.at[place + d], 1)
            for q in range(Q):
                spread(q, d).start()

        @pl.loop(jnp.maximum(LATE - place, 1), nz - place)
        def _(d):
            pl.semaphore_wait(above.at[place + d], 1)
            spread(0, d).start()

        for q in range(1, Q):
            for d in outward:
                @pl.when(jnp.logical_and(place + d >= LATE, place + d < nz))
                def _():
                    spread(q, d).start()

    with jax.named_scope("late"):
        @pl.when(place >= EARLY)
        def _():
            prepare()

    for q in range(Q):
        with jax.named_scope("mid%d" % q):
            settle(mids[q].at[pl.ds(0, nt * (nz - 1))], r1.at[q])

        pltpu.make_async_copy(share(q, z), mids[q].at[pl.ds(nt * z, nt)], own_sem.at[q]).wait()

        @pl.loop(1, nz)
        def _(d):
            for tl in range(nt):
                mail[q, d, tl] = mids[q][rank[nt * far(d) + tl]]

        for tl in range(nt):
            gathered[q, tl, pl.ds(pl.multiple_of(z * chunk, 8), chunk), :] = mids[q][rank[nt * z + tl]]

        for d in outward:
            deliver(q, d).start()

    contract = (((1,), (1,)), ((), ()))
    ks = nz * keep
    colours = depth // 4

    def target(o):
        return lax.rem(x + o, half)

    def reduce_copy(q, o, core):
        xs = target(o)
        return pltpu.make_async_remote_copy(
            src_ref=part.at[q, xs * nc + core], dst_ref=parts.at[q, x],
            send_sem=s3.at[q], recv_sem=r3.at[q],
            device_id={"xyz": half * c + xs, "src": core}, device_id_type=MESH)

    sender = lax.div(x, half)
    step = ks // half
    per = relays // 2
    piece = step // per

    def relay_at(i):
        return lax.rem(i + nz - BEFORE, nz)

    my_relay = lax.rem(z + BEFORE, nz)

    def contract_chunk(q):
        with jax.named_scope("got%d" % q):
            settle(gathered.at[q, :, pl.ds(0, (nz - 1) * chunk)], r2.at[q])

        for tl in range(nt):
            for i in range(colours):
                for b in range(2):
                    re = gathered[q, tl, pl.ds(i * 4 + b * 2, ks, stride=depth), :]
                    im = gathered[q, tl, pl.ds(i * 4 + b * 2 + 1, ks, stride=depth), :]
                    g = i * 2 + b
                    for at, value in ((0, re), (depth // 2, im)):
                        top = value.astype(jnp.bfloat16)
                        rest = (value - top.astype(jnp.float32)).astype(jnp.bfloat16)
                        where = slice((at + g) * LANES, (at + g + 1) * LANES)
                        cross = slice((depth // 2 - at + g) * LANES, (depth // 2 - at + g + 1) * LANES)
                        left[0:ks, where] = top
                        left[2 * ks:3 * ks, where] = rest
                        left[ks:2 * ks, cross] = top if at == 0 else -top
                        left[3 * ks:4 * ks, cross] = rest if at == 0 else -rest
            one = lax.dot_general(left[...], high[tl], contract, preferred_element_type=jnp.float32)
            two = lax.dot_general(left[0:2 * ks, :], low[tl], contract, preferred_element_type=jnp.float32)
            total = one[0:2 * ks] + one[2 * ks:4 * ks] + two
            for xs in range(half):
                for core in range(nc):
                    for reim in range(2):
                        part[q, xs * nc + core, tl, reim] = total[reim * ks + xs * step:reim * ks + (xs + 1) * step, core * rows:(core + 1) * rows]

        for o in [0] + sorted(range(1, half), key=lambda o: abs(2 * o - half)):
            for core in range(nc):
                mine = jnp.logical_and(half * c + target(o) == x, c == core)

                @pl.when(jnp.logical_not(mine))
                def _():
                    reduce_copy(q, o, core).start()

                if o == 0:
                    @pl.when(mine)
                    def _():
                        parts[q, x] = part[q, target(o) * nc + core]

    def return_copy(q, i):
        return pltpu.make_async_remote_copy(
            src_ref=home.at[q, i], dst_ref=relay[q].at[pl.ds(nt * z, nt)],
            send_sem=s4.at[q], recv_sem=r4.at[q], device_id={"ta": relay_at(i)}, device_id_type=MESH)

    def final_copy(q, there):
        return pltpu.make_async_remote_copy(
            src_ref=post.at[q, there], dst_ref=back.at[q, my_relay],
            send_sem=s5.at[q], recv_sem=r5.at[q], device_id={"ta": there}, device_id_type=MESH)

    def reduce_chunk(q):
        with jax.named_scope("reduced%d" % q):
            @pl.when(sender == c)
            def _():
                settle(parts.at[q, pl.ds(0, nx - 1)], r3.at[q])

            @pl.when(sender != c)
            def _():
                settle(parts.at[q], r3.at[q])

        for tl in range(nt):
            for reim in range(2):
                total = parts[q, 0, tl, reim]
                for xs in range(1, nx):
                    total += parts[q, xs, tl, reim]
                for i in range(per):
                    home[q, reim * per + i, tl] = total[i * piece:(i + 1) * piece, :]

        for i in range(relays):
            @pl.when(relay_at(i) != z)
            def _():
                return_copy(q, i).start()

            @pl.when(relay_at(i) == z)
            def _():
                for tl in range(nt):
                    relay[q][nt * z + tl] = home[q, i, tl]

    def relay_chunk(q):
        @pl.when(my_relay < relays)
        def _():
            with jax.named_scope("relayed%d" % q):
                settle(relay[q].at[pl.ds(0, nt * (nz - 1))], r4.at[q])

            for there in range(nz):
                for tl in range(nt):
                    post[q, there, tl] = relay[q][order[nt * there + tl]]

                @pl.when(there != z)
                def _():
                    final_copy(q, there).start()

            back[q, my_relay] = post[q, z]

    for q in range(Q):
        contract_chunk(q)
        reduce_chunk(q)
    for q in range(Q):
        relay_chunk(q)

    for q in range(Q):
        settle(mids[q].at[pl.ds(0, nt * (nz - 1))], s1.at[q])
        settle(mail.at[q, pl.ds(0, nz - 1)], s2.at[q])

        @pl.when(sender == c)
        def _():
            settle(part.at[q, pl.ds(0, nx - 1)], s3.at[q])

        @pl.when(sender != c)
        def _():
            settle(part.at[q], s3.at[q])

        @pl.when(my_relay < relays)
        def _():
            settle(home.at[q, pl.ds(0, relays - 1)], s4.at[q])
            settle(post.at[q, pl.ds(0, nz - 1)], s5.at[q])

        @pl.when(my_relay >= relays)
        def _():
            settle(home.at[q], s4.at[q])

    for q in range(Q):
        with jax.named_scope("final%d" % q):
            @pl.when(my_relay < relays)
            def _():
                settle(back.at[q, pl.ds(0, relays - 1)], r5.at[q])

            @pl.when(my_relay >= relays)
            def _():
                settle(back.at[q], r5.at[q])

        with jax.named_scope("asm%d" % q):
            for reim in range(2):
                for i in range(per):
                    for tl in range(nt):
                        got = back[q, reim * per + i, tl]
                        for j in range(piece // keep):
                            at = (i * (piece // keep) + j) * Q * keep + q * keep
                            flat[tl, reim, at:at + keep, :] = got[j * keep:(j + 1) * keep, :]

    with jax.named_scope("outs"):
        for s in range(spin):
            out_ref[:, :, s] = flat[:, :, :, s * ns:(s + 1) * ns]


def solution(mesh):
    nz, nx, nc = mesh.shape["ta"], mesh.shape["xyz"], mesh.shape["src"]

    def local(spinors, eigvecs, group_of, source_ids):
        ns, nt, _, spin, colours, sites = spinors.shape
        kk = eigvecs.shape[1]
        blocks = sites // LANES
        depth = 2 * colours * blocks
        keep = kk // (nc * nz * Q)
        rows = ns * spin
        ks = nz * keep
        spin_view = spinors.transpose(0, 1, 2, 4, 3, 5).reshape(ns, nt, 2, colours, spin, blocks, LANES)
        spin_view = spin_view.transpose(0, 1, 2, 3, 5, 4, 6).reshape(ns, nt, depth * spin, LANES)
        vec_view = eigvecs.transpose(0, 1, 3, 2, 4).reshape(nt, kk, colours, 2, blocks, LANES)
        vec_view = vec_view.transpose(0, 1, 2, 4, 3, 5).reshape(nt, kk * depth, LANES)
        step = ks * nc // nx
        relays = RELAYS
        sizes = (nz, nx, nc, ns, nt, spin, depth, keep, relays)
        f32, bf16 = jnp.float32, jnp.bfloat16
        dma = pltpu.SemaphoreType.DMA
        small = (step * 2 // relays, LANES)
        out = pl.pallas_call(
            functools.partial(kernel, sizes),
            out_shape=jax.ShapeDtypeStruct((nt, 2, spin, kk // nx, ns), f32),
            in_specs=[pl.BlockSpec(memory_space=pl.ANY)] * 4,
            out_specs=pl.BlockSpec(memory_space=pltpu.VMEM),
            scratch_shapes=[
                pltpu.SMEM((nz * nt,), jnp.int32),
                pltpu.SMEM((ns,), jnp.int32),
                pltpu.SMEM((nz * nt,), jnp.int32),
                pltpu.SMEM((nz * nt,), jnp.int32),
                pltpu.SMEM((ns,), jnp.int32),
                pltpu.VMEM((ns, nt, depth * spin, LANES), f32),
                pltpu.VMEM((nc, nt, depth, rows, LANES), f32),
                pltpu.VMEM((nt, nc * rows, depth * LANES), bf16),
                pltpu.VMEM((nt, nc * rows, depth * LANES), bf16),
                [pltpu.VMEM((nz * nt, keep * depth, LANES), f32)] * Q,
                pltpu.VMEM((Q, nz, nt, keep * depth, LANES), f32),
                pltpu.VMEM((Q, nt, ks * depth, LANES), f32),
                pltpu.VMEM((4 * ks, depth * LANES), bf16),
                pltpu.VMEM((Q, nx, nt, 2, ks * nc // nx, LANES), f32),
                pltpu.VMEM((Q, nx, nt, 2, ks * nc // nx, LANES), f32),
                pltpu.VMEM((Q, relays, nt) + small, f32),
                [pltpu.VMEM((nz * nt,) + small, f32)] * Q,
                pltpu.VMEM((Q, nz, nt) + small, f32),
                pltpu.VMEM((Q, relays, nt) + small, f32),
                pltpu.VMEM((nt, 2, kk // nx, rows), f32),
                pltpu.SemaphoreType.REGULAR((nz,)), pltpu.SemaphoreType.REGULAR((2, nx // 2 - 1)), dma((2,)), dma, dma((Q,)), dma((2,)),
                [dma((Q,))] * 2, [dma((Q,))] * 2, [dma((Q,))] * 2, [dma((Q,))] * 2, [dma((Q,))] * 2,
            ],
            compiler_params=pltpu.CompilerParams(collective_id=0, has_side_effects=True),
        )(group_of, source_ids, vec_view, spin_view)
        return out.transpose(0, 1, 2, 4, 3)

    in_specs = (
        P("src", "ta", None, "job", None, "xyz"),
        P("ta", "job", None, None, "xyz"),
        P(),
        P("src"),
    )
    out_specs = P("ta", None, "job", "src", "xyz")
    return jax.shard_map(local, mesh=mesh, in_specs=in_specs, out_specs=out_specs, check_vma=False)
```

```python
import functools

import jax
import jax.numpy as jnp
from jax import lax
from jax.experimental import pallas as pl
from jax.experimental.pallas import tpu as pltpu
from jax.sharding import PartitionSpec as P

MESH = pl.DeviceIdType.MESH
LANES = 128
Q = 2
EARLY = 12
LATE = 0
RELAYS = 4
BEFORE = 3


def kernel(sizes, group_hbm, ids_hbm, vec_ref, spin_ref, out_ref,
           group_ref, ids_ref, rank, order, inverse, raw, both, high, low, mids, mail, gathered, left,
           part, parts, home, relay, post, back, flat,
           above, along, small_sem, load_sem, own_sem, pair_sem, *pairs):
    (s1, r1), (s2, r2), (s3, r3), (s4, r4), (s5, r5) = pairs
    nz, nx, nc, ns, nt, spin, depth, keep, relays = sizes
    z, x, c = lax.axis_index("ta"), lax.axis_index("xyz"), lax.axis_index("src")
    other = 1 - c
    rows = ns * spin
    chunk = keep * depth
    half = nx // nc

    def far(d):
        return lax.rem(z + d, nz)

    def settle(ref, sem):
        pltpu.make_async_copy(ref, ref, sem).wait()

    place = lax.rem(z + nz - 1, nz)

    def at_place(p):
        return lax.rem(p + 1, nz)

    barrier = pltpu.get_barrier_semaphore()

    @pl.loop(0, nz - 1 - place)
    def _(i):
        pl.semaphore_signal(barrier, inc=1, device_id={"ta": at_place(nz - 1 - i)}, device_id_type=MESH)

    right, left_x = lax.rem(x + 1, nx), lax.rem(x + nx - 1, nx)
    for there in (right, left_x):
        pl.semaphore_signal(barrier, inc=1, device_id={"xyz": there}, device_id_type=MESH)
    pl.semaphore_signal(barrier, inc=1, device_id={"src": other}, device_id_type=MESH)

    loads = [
        pltpu.make_async_copy(group_hbm, group_ref, small_sem.at[0]),
        pltpu.make_async_copy(ids_hbm, ids_ref, small_sem.at[1]),
        pltpu.make_async_copy(spin_ref, raw, load_sem),
    ]
    for load in loads:
        load.start()
    pl.semaphore_wait(barrier, 3 + place)

    def share(q, there):
        first = (c * (nz * Q * keep) + there * (Q * keep) + q * keep) * depth
        return vec_ref.at[:, pl.ds(pl.multiple_of(first, 8), chunk), :]

    def spread(q, d):
        return pltpu.make_async_remote_copy(
            src_ref=share(q, far(d)), dst_ref=mids[q].at[pl.ds(nt * z, nt)],
            send_sem=s1.at[q], recv_sem=r1.at[q], device_id={"ta": far(d)}, device_id_type=MESH)

    def deliver(q, d):
        return pltpu.make_async_remote_copy(
            src_ref=mail.at[q, d], dst_ref=gathered.at[q, :, pl.ds(pl.multiple_of(z * chunk, 8), chunk), :],
            send_sem=s2.at[q], recv_sem=r2.at[q], device_id={"ta": far(d)}, device_id_type=MESH)

    outward = sorted(range(1, nz), key=lambda d: -min(d, nz - d))
    with jax.named_scope("known"):
      for d in outward:
        @pl.when(d >= nz - place)
        def _():
            pl.semaphore_signal(above.at[place], inc=1, device_id={"ta": far(d)}, device_id_type=MESH)

    for q in range(Q):
        for d in outward:
            @pl.when(d >= nz - place)
            def _():
                spread(q, d).start()

        pltpu.make_async_copy(share(q, z), mids[q].at[pl.ds(nt * z, nt)], own_sem.at[q]).start()

    count = nz * nt

    def prepare():
        hops = list(range(nx // 2 - 1))

        def tell(j):
            pl.semaphore_signal(along.at[0, j], inc=1, device_id={"xyz": left_x}, device_id_type=MESH)
            pl.semaphore_signal(along.at[1, j], inc=1, device_id={"xyz": right}, device_id_type=MESH)

        def hear(j):
            pl.semaphore_wait(along.at[0, j], 1)
            pl.semaphore_wait(along.at[1, j], 1)

        tell(hops[0])
        loads[0].wait()
        loads[1].wait()


        @pl.loop(0, count)
        def _(t):
            mine = group_ref[t] * count + t
            total = jnp.int32(0)
            for u in range(count):
                total += jnp.where(group_ref[u] * count + u < mine, 1, 0)
            rank[t] = total

        @pl.loop(0, count)
        def _(r):
            total = jnp.int32(0)
            for u in range(count):
                total = jnp.maximum(total, jnp.where(rank[u] == r, u, 0))
            order[r] = total

        @pl.loop(0, ns)
        def _(j):
            total = jnp.int32(0)
            for u in range(ns):
                total = jnp.maximum(total, jnp.where(ids_ref[u] - c * ns == j, u, 0))
            inverse[j] = total

        for j in hops[:-1]:
            hear(j)
            tell(j + 1)
        loads[2].wait()

        @pl.loop(0, ns)
        def _(j):
            n = inverse[j]
            for tl in range(nt):
                for g in range(depth):
                    for s in range(spin):
                        both[c, tl, g, pl.ds(s * ns + j, 1), :] = raw[n, tl, g * spin + s:g * spin + s + 1, :]

        pair = pltpu.make_async_remote_copy(
            src_ref=both.at[c], dst_ref=both.at[c], send_sem=pair_sem.at[0], recv_sem=pair_sem.at[1],
            device_id={"src": other}, device_id_type=MESH)
        hear(hops[-1])
        pair.start()
        pair.wait()

        @pl.loop(0, nt)
        def _(tl):
            for core in range(nc):
                for g in range(depth):
                    block = both[core, tl, g]
                    top = block.astype(jnp.bfloat16)
                    high[tl, core * rows:(core + 1) * rows, g * LANES:(g + 1) * LANES] = top
                    low[tl, core * rows:(core + 1) * rows, g * LANES:(g + 1) * LANES] = (block - top.astype(jnp.float32)).astype(jnp.bfloat16)

    with jax.named_scope("early"):
        @pl.when(place < EARLY)
        def _():
            prepare()

    with jax.named_scope("upper"):
        @pl.loop(1, jnp.maximum(LATE - place, 1))
        def _(d):
            pl.semaphore_wait(above.at[place + d], 1)
            for q in range(Q):
                spread(q, d).start()

        @pl.loop(jnp.maximum(LATE - place, 1), nz - place)
        def _(d):
            pl.semaphore_wait(above.at[place + d], 1)
            spread(0, d).start()

        for q in range(1, Q):
            for d in outward:
                @pl.when(jnp.logical_and(place + d >= LATE, place + d < nz))
                def _():
                    spread(q, d).start()

    with jax.named_scope("late"):
        @pl.when(place >= EARLY)
        def _():
            prepare()

    for q in range(Q):
        with jax.named_scope("mid%d" % q):
            settle(mids[q].at[pl.ds(0, nt * (nz - 1))], r1.at[q])

        pltpu.make_async_copy(share(q, z), mids[q].at[pl.ds(nt * z, nt)], own_sem.at[q]).wait()

        @pl.loop(1, nz)
        def _(d):
            for tl in range(nt):
                mail[q, d, tl] = mids[q][rank[nt * far(d) + tl]]

        for tl in range(nt):
            gathered[q, tl, pl.ds(pl.multiple_of(z * chunk, 8), chunk), :] = mids[q][rank[nt * z + tl]]

        for d in outward:
            deliver(q, d).start()

    contract = (((1,), (1,)), ((), ()))
    ks = nz * keep
    colours = depth // 4

    def target(o):
        return lax.rem(x + o, half)

    def reduce_copy(q, o, core, tl):
        xs = target(o)
        return pltpu.make_async_remote_copy(
            src_ref=part.at[q, xs * nc + core, tl], dst_ref=parts.at[q, x, tl],
            send_sem=s3.at[q], recv_sem=r3.at[q],
            device_id={"xyz": half * c + xs, "src": core}, device_id_type=MESH)

    sender = lax.div(x, half)
    step = ks // half
    per = relays // 2
    piece = step // per

    def relay_at(i):
        return lax.rem(i + nz - BEFORE, nz)

    my_relay = lax.rem(z + BEFORE, nz)

    def contract_chunk(q):
        with jax.named_scope("got%d" % q):
            settle(gathered.at[q, :, pl.ds(0, (nz - 1) * chunk)], r2.at[q])

        for tl in range(nt):
            for i in range(colours):
                for b in range(2):
                    re = gathered[q, tl, pl.ds(i * 4 + b * 2, ks, stride=depth), :]
                    im = gathered[q, tl, pl.ds(i * 4 + b * 2 + 1, ks, stride=depth), :]
                    g = i * 2 + b
                    for at, value in ((0, re), (depth // 2, im)):
                        top = value.astype(jnp.bfloat16)
                        rest = (value - top.astype(jnp.float32)).astype(jnp.bfloat16)
                        where = slice((at + g) * LANES, (at + g + 1) * LANES)
                        cross = slice((depth // 2 - at + g) * LANES, (depth // 2 - at + g + 1) * LANES)
                        left[0:ks, where] = top
                        left[2 * ks:3 * ks, where] = rest
                        left[ks:2 * ks, cross] = top if at == 0 else -top
                        left[3 * ks:4 * ks, cross] = rest if at == 0 else -rest
            one = lax.dot_general(left[...], high[tl], contract, preferred_element_type=jnp.float32)
            two = lax.dot_general(left[0:2 * ks, :], low[tl], contract, preferred_element_type=jnp.float32)
            total = one[0:2 * ks] + one[2 * ks:4 * ks] + two
            for xs in range(half):
                for core in range(nc):
                    for reim in range(2):
                        part[q, xs * nc + core, tl, reim] = total[reim * ks + xs * step:reim * ks + (xs + 1) * step, core * rows:(core + 1) * rows]

            for o in [0] + sorted(range(1, half), key=lambda o: abs(2 * o - half)):
                for core in range(nc):
                    mine = jnp.logical_and(half * c + target(o) == x, c == core)

                    @pl.when(jnp.logical_not(mine))
                    def _():
                        reduce_copy(q, o, core, tl).start()

                    if o == 0:
                        @pl.when(mine)
                        def _():
                            parts[q, x, tl] = part[q, target(o) * nc + core, tl]

    def return_copy(q, i):
        return pltpu.make_async_remote_copy(
            src_ref=home.at[q, i], dst_ref=relay[q].at[pl.ds(nt * z, nt)],
            send_sem=s4.at[q], recv_sem=r4.at[q], device_id={"ta": relay_at(i)}, device_id_type=MESH)

    def final_copy(q, there):
        return pltpu.make_async_remote_copy(
            src_ref=post.at[q, there], dst_ref=back.at[q, my_relay],
            send_sem=s5.at[q], recv_sem=r5.at[q], device_id={"ta": there}, device_id_type=MESH)

    def reduce_chunk(q):
        with jax.named_scope("reduced%d" % q):
            @pl.when(sender == c)
            def _():
                settle(parts.at[q, pl.ds(0, nx - 1)], r3.at[q])

            @pl.when(sender != c)
            def _():
                settle(parts.at[q], r3.at[q])

        for tl in range(nt):
            for reim in range(2):
                total = parts[q, 0, tl, reim]
                for xs in range(1, nx):
                    total += parts[q, xs, tl, reim]
                for i in range(per):
                    home[q, reim * per + i, tl] = total[i * piece:(i + 1) * piece, :]

        for i in range(relays):
            @pl.when(relay_at(i) != z)
            def _():
                return_copy(q, i).start()

            @pl.when(relay_at(i) == z)
            def _():
                for tl in range(nt):
                    relay[q][nt * z + tl] = home[q, i, tl]

    def relay_chunk(q):
        @pl.when(my_relay < relays)
        def _():
            with jax.named_scope("relayed%d" % q):
                settle(relay[q].at[pl.ds(0, nt * (nz - 1))], r4.at[q])

            for there in range(nz):
                for tl in range(nt):
                    post[q, there, tl] = relay[q][order[nt * there + tl]]

                @pl.when(there != z)
                def _():
                    final_copy(q, there).start()

            back[q, my_relay] = post[q, z]

    for q in range(Q):
        contract_chunk(q)
    for q in range(Q):
        reduce_chunk(q)
    for q in range(Q):
        relay_chunk(q)

    for q in range(Q):
        settle(mids[q].at[pl.ds(0, nt * (nz - 1))], s1.at[q])
        settle(mail.at[q, pl.ds(0, nz - 1)], s2.at[q])

        @pl.when(sender == c)
        def _():
            settle(part.at[q, pl.ds(0, nx - 1)], s3.at[q])

        @pl.when(sender != c)
        def _():
            settle(part.at[q], s3.at[q])

        @pl.when(my_relay < relays)
        def _():
            settle(home.at[q, pl.ds(0, relays - 1)], s4.at[q])
            settle(post.at[q, pl.ds(0, nz - 1)], s5.at[q])

        @pl.when(my_relay >= relays)
        def _():
            settle(home.at[q], s4.at[q])

    for q in range(Q):
        with jax.named_scope("final%d" % q):
            @pl.when(my_relay < relays)
            def _():
                settle(back.at[q, pl.ds(0, relays - 1)], r5.at[q])

            @pl.when(my_relay >= relays)
            def _():
                settle(back.at[q], r5.at[q])

        with jax.named_scope("asm%d" % q):
            for reim in range(2):
                for i in range(per):
                    for tl in range(nt):
                        got = back[q, reim * per + i, tl]
                        for j in range(piece // keep):
                            at = (i * (piece // keep) + j) * Q * keep + q * keep
                            flat[tl, reim, at:at + keep, :] = got[j * keep:(j + 1) * keep, :]

    with jax.named_scope("outs"):
        for s in range(spin):
            out_ref[:, :, s] = flat[:, :, :, s * ns:(s + 1) * ns]


def solution(mesh):
    nz, nx, nc = mesh.shape["ta"], mesh.shape["xyz"], mesh.shape["src"]

    def local(spinors, eigvecs, group_of, source_ids):
        ns, nt, _, spin, colours, sites = spinors.shape
        kk = eigvecs.shape[1]
        blocks = sites // LANES
        depth = 2 * colours * blocks
        keep = kk // (nc * nz * Q)
        rows = ns * spin
        ks = nz * keep
        spin_view = spinors.transpose(0, 1, 2, 4, 3, 5).reshape(ns, nt, 2, colours, spin, blocks, LANES)
        spin_view = spin_view.transpose(0, 1, 2, 3, 5, 4, 6).reshape(ns, nt, depth * spin, LANES)
        vec_view = eigvecs.transpose(0, 1, 3, 2, 4).reshape(nt, kk, colours, 2, blocks, LANES)
        vec_view = vec_view.transpose(0, 1, 2, 4, 3, 5).reshape(nt, kk * depth, LANES)
        step = ks * nc // nx
        relays = RELAYS
        sizes = (nz, nx, nc, ns, nt, spin, depth, keep, relays)
        f32, bf16 = jnp.float32, jnp.bfloat16
        dma = pltpu.SemaphoreType.DMA
        small = (step * 2 // relays, LANES)
        out = pl.pallas_call(
            functools.partial(kernel, sizes),
            out_shape=jax.ShapeDtypeStruct((nt, 2, spin, kk // nx, ns), f32),
            in_specs=[pl.BlockSpec(memory_space=pl.ANY)] * 4,
            out_specs=pl.BlockSpec(memory_space=pltpu.VMEM),
            scratch_shapes=[
                pltpu.SMEM((nz * nt,), jnp.int32),
                pltpu.SMEM((ns,), jnp.int32),
                pltpu.SMEM((nz * nt,), jnp.int32),
                pltpu.SMEM((nz * nt,), jnp.int32),
                pltpu.SMEM((ns,), jnp.int32),
                pltpu.VMEM((ns, nt, depth * spin, LANES), f32),
                pltpu.VMEM((nc, nt, depth, rows, LANES), f32),
                pltpu.VMEM((nt, nc * rows, depth * LANES), bf16),
                pltpu.VMEM((nt, nc * rows, depth * LANES), bf16),
                [pltpu.VMEM((nz * nt, keep * depth, LANES), f32)] * Q,
                pltpu.VMEM((Q, nz, nt, keep * depth, LANES), f32),
                pltpu.VMEM((Q, nt, ks * depth, LANES), f32),
                pltpu.VMEM((4 * ks, depth * LANES), bf16),
                pltpu.VMEM((Q, nx, nt, 2, ks * nc // nx, LANES), f32),
                pltpu.VMEM((Q, nx, nt, 2, ks * nc // nx, LANES), f32),
                pltpu.VMEM((Q, relays, nt) + small, f32),
                [pltpu.VMEM((nz * nt,) + small, f32)] * Q,
                pltpu.VMEM((Q, nz, nt) + small, f32),
                pltpu.VMEM((Q, relays, nt) + small, f32),
                pltpu.VMEM((nt, 2, kk // nx, rows), f32),
                pltpu.SemaphoreType.REGULAR((nz,)), pltpu.SemaphoreType.REGULAR((2, nx // 2 - 1)), dma((2,)), dma, dma((Q,)), dma((2,)),
                [dma((Q,))] * 2, [dma((Q,))] * 2, [dma((Q,))] * 2, [dma((Q,))] * 2, [dma((Q,))] * 2,
            ],
            compiler_params=pltpu.CompilerParams(collective_id=0, has_side_effects=True),
        )(group_of, source_ids, vec_view, spin_view)
        return out.transpose(0, 1, 2, 4, 3)

    in_specs = (
        P("src", "ta", None, "job", None, "xyz"),
        P("ta", "job", None, None, "xyz"),
        P(),
        P("src"),
    )
    out_specs = P("ta", None, "job", "src", "xyz")
    return jax.shard_map(local, mesh=mesh, in_specs=in_specs, out_specs=out_specs, check_vma=False)
```

```python
import functools

import jax
import jax.numpy as jnp
from jax import lax
from jax.experimental import pallas as pl
from jax.experimental.pallas import tpu as pltpu
from jax.sharding import PartitionSpec as P

MESH = pl.DeviceIdType.MESH
LANES = 128
Q = 2
EARLY = 9
LATE = 0
RELAYS = 4
BEFORE = 3


def kernel(sizes, group_hbm, ids_hbm, vec_ref, spin_ref, out_ref,
           group_ref, ids_ref, rank, order, inverse, raw, both, high, low, mids, mail, gathered, left,
           part, parts, home, relay, post, back, flat,
           above, along, small_sem, load_sem, own_sem, pair_sem, *pairs):
    (s1, r1), (s2, r2), (s3, r3), (s4, r4), (s5, r5) = pairs
    nz, nx, nc, ns, nt, spin, depth, keep, relays = sizes
    z, x, c = lax.axis_index("ta"), lax.axis_index("xyz"), lax.axis_index("src")
    other = 1 - c
    rows = ns * spin
    chunk = keep * depth
    half = nx // nc

    def far(d):
        return lax.rem(z + d, nz)

    def settle(ref, sem):
        pltpu.make_async_copy(ref, ref, sem).wait()

    place = lax.rem(z + nz - 1, nz)

    def at_place(p):
        return lax.rem(p + 1, nz)

    barrier = pltpu.get_barrier_semaphore()

    @pl.loop(0, nz - 1 - place)
    def _(i):
        pl.semaphore_signal(barrier, inc=1, device_id={"ta": at_place(nz - 1 - i)}, device_id_type=MESH)

    right, left_x = lax.rem(x + 1, nx), lax.rem(x + nx - 1, nx)
    for there in (right, left_x):
        pl.semaphore_signal(barrier, inc=1, device_id={"xyz": there}, device_id_type=MESH)
    pl.semaphore_signal(barrier, inc=1, device_id={"src": other}, device_id_type=MESH)

    loads = [
        pltpu.make_async_copy(group_hbm, group_ref, small_sem.at[0]),
        pltpu.make_async_copy(ids_hbm, ids_ref, small_sem.at[1]),
        pltpu.make_async_copy(spin_ref, raw, load_sem),
    ]
    for load in loads:
        load.start()
    pl.semaphore_wait(barrier, 3 + place)

    def share(q, there):
        first = (c * (nz * Q * keep) + there * (Q * keep) + q * keep) * depth
        return vec_ref.at[:, pl.ds(pl.multiple_of(first, 8), chunk), :]

    def spread(q, d):
        return pltpu.make_async_remote_copy(
            src_ref=share(q, far(d)), dst_ref=mids[q].at[pl.ds(nt * z, nt)],
            send_sem=s1.at[q], recv_sem=r1.at[q], device_id={"ta": far(d)}, device_id_type=MESH)

    def deliver(q, d):
        return pltpu.make_async_remote_copy(
            src_ref=mail.at[q, d], dst_ref=gathered.at[q, :, pl.ds(pl.multiple_of(z * chunk, 8), chunk), :],
            send_sem=s2.at[q], recv_sem=r2.at[q], device_id={"ta": far(d)}, device_id_type=MESH)

    outward = sorted(range(1, nz), key=lambda d: -min(d, nz - d))
    with jax.named_scope("known"):
      for d in outward:
        @pl.when(d >= nz - place)
        def _():
            pl.semaphore_signal(above.at[place], inc=1, device_id={"ta": far(d)}, device_id_type=MESH)

    for q in range(Q):
        for d in outward:
            @pl.when(d >= nz - place)
            def _():
                spread(q, d).start()

        pltpu.make_async_copy(share(q, z), mids[q].at[pl.ds(nt * z, nt)], own_sem.at[q]).start()

    count = nz * nt

    def prepare():
        hops = list(range(nx // 2 - 1))

        def tell(j):
            pl.semaphore_signal(along.at[0, j], inc=1, device_id={"xyz": left_x}, device_id_type=MESH)
            pl.semaphore_signal(along.at[1, j], inc=1, device_id={"xyz": right}, device_id_type=MESH)

        def hear(j):
            pl.semaphore_wait(along.at[0, j], 1)
            pl.semaphore_wait(along.at[1, j], 1)

        tell(hops[0])
        loads[0].wait()
        loads[1].wait()


        @pl.loop(0, count)
        def _(t):
            mine = group_ref[t] * count + t
            total = jnp.int32(0)
            for u in range(count):
                total += jnp.where(group_ref[u] * count + u < mine, 1, 0)
            rank[t] = total

        @pl.loop(0, count)
        def _(r):
            total = jnp.int32(0)
            for u in range(count):
                total = jnp.maximum(total, jnp.where(rank[u] == r, u, 0))
            order[r] = total

        @pl.loop(0, ns)
        def _(j):
            total = jnp.int32(0)
            for u in range(ns):
                total = jnp.maximum(total, jnp.where(ids_ref[u] - c * ns == j, u, 0))
            inverse[j] = total

        for j in hops[:-1]:
            hear(j)
            tell(j + 1)
        loads[2].wait()

        @pl.loop(0, ns)
        def _(j):
            n = inverse[j]
            for tl in range(nt):
                for g in range(depth):
                    for s in range(spin):
                        both[c, tl, g, pl.ds(s * ns + j, 1), :] = raw[n, tl, g * spin + s:g * spin + s + 1, :]

        pair = pltpu.make_async_remote_copy(
            src_ref=both.at[c], dst_ref=both.at[c], send_sem=pair_sem.at[0], recv_sem=pair_sem.at[1],
            device_id={"src": other}, device_id_type=MESH)
        hear(hops[-1])
        pair.start()
        pair.wait()

        @pl.loop(0, nt)
        def _(tl):
            for core in range(nc):
                for g in range(depth):
                    block = both[core, tl, g]
                    top = block.astype(jnp.bfloat16)
                    high[tl, core * rows:(core + 1) * rows, g * LANES:(g + 1) * LANES] = top
                    low[tl, core * rows:(core + 1) * rows, g * LANES:(g + 1) * LANES] = (block - top.astype(jnp.float32)).astype(jnp.bfloat16)

    with jax.named_scope("early"):
        @pl.when(place < EARLY)
        def _():
            prepare()

    with jax.named_scope("upper"):
        @pl.loop(1, jnp.maximum(LATE - place, 1))
        def _(d):
            pl.semaphore_wait(above.at[place + d], 1)
            for q in range(Q):
                spread(q, d).start()

        @pl.loop(jnp.maximum(LATE - place, 1), nz - place)
        def _(d):
            pl.semaphore_wait(above.at[place + d], 1)
            spread(0, d).start()

        for q in range(1, Q):
            for d in outward:
                @pl.when(jnp.logical_and(place + d >= LATE, place + d < nz))
                def _():
                    spread(q, d).start()

    with jax.named_scope("late"):
        @pl.when(place >= EARLY)
        def _():
            prepare()

    for q in range(Q):
        with jax.named_scope("mid%d" % q):
            settle(mids[q].at[pl.ds(0, nt * (nz - 1))], r1.at[q])

        pltpu.make_async_copy(share(q, z), mids[q].at[pl.ds(nt * z, nt)], own_sem.at[q]).wait()

        @pl.loop(1, nz)
        def _(d):
            for tl in range(nt):
                mail[q, d, tl] = mids[q][rank[nt * far(d) + tl]]

        for tl in range(nt):
            gathered[q, tl, pl.ds(pl.multiple_of(z * chunk, 8), chunk), :] = mids[q][rank[nt * z + tl]]

        for d in outward:
            deliver(q, d).start()

    contract = (((1,), (1,)), ((), ()))
    ks = nz * keep
    colours = depth // 4

    def target(o):
        return lax.rem(x + o, half)

    def reduce_copy(q, o, core, tl):
        xs = target(o)
        return pltpu.make_async_remote_copy(
            src_ref=part.at[q, xs * nc + core, tl], dst_ref=parts.at[q, x, tl],
            send_sem=s3.at[q], recv_sem=r3.at[q],
            device_id={"xyz": half * c + xs, "src": core}, device_id_type=MESH)

    sender = lax.div(x, half)
    step = ks // half
    per = relays // 2
    piece = step // per

    def relay_at(i):
        return lax.rem(i + nz - BEFORE, nz)

    my_relay = lax.rem(z + BEFORE, nz)

    def contract_chunk(q):
        with jax.named_scope("got%d" % q):
            settle(gathered.at[q, :, pl.ds(0, (nz - 1) * chunk)], r2.at[q])

        for tl in range(nt):
            for i in range(colours):
                for b in range(2):
                    re = gathered[q, tl, pl.ds(i * 4 + b * 2, ks, stride=depth), :]
                    im = gathered[q, tl, pl.ds(i * 4 + b * 2 + 1, ks, stride=depth), :]
                    g = i * 2 + b
                    for at, value in ((0, re), (depth // 2, im)):
                        top = value.astype(jnp.bfloat16)
                        rest = (value - top.astype(jnp.float32)).astype(jnp.bfloat16)
                        where = slice((at + g) * LANES, (at + g + 1) * LANES)
                        cross = slice((depth // 2 - at + g) * LANES, (depth // 2 - at + g + 1) * LANES)
                        left[0:ks, where] = top
                        left[2 * ks:3 * ks, where] = rest
                        left[ks:2 * ks, cross] = top if at == 0 else -top
                        left[3 * ks:4 * ks, cross] = rest if at == 0 else -rest
            one = lax.dot_general(left[...], high[tl], contract, preferred_element_type=jnp.float32)
            two = lax.dot_general(left[0:2 * ks, :], low[tl], contract, preferred_element_type=jnp.float32)
            total = one[0:2 * ks] + one[2 * ks:4 * ks] + two
            for xs in range(half):
                for core in range(nc):
                    for reim in range(2):
                        part[q, xs * nc + core, tl, reim] = total[reim * ks + xs * step:reim * ks + (xs + 1) * step, core * rows:(core + 1) * rows]

            for o in [0] + sorted(range(1, half), key=lambda o: abs(2 * o - half)):
                for core in range(nc):
                    mine = jnp.logical_and(half * c + target(o) == x, c == core)

                    @pl.when(jnp.logical_not(mine))
                    def _():
                        reduce_copy(q, o, core, tl).start()

                    if o == 0:
                        @pl.when(mine)
                        def _():
                            parts[q, x, tl] = part[q, target(o) * nc + core, tl]

    def return_copy(q, i):
        return pltpu.make_async_remote_copy(
            src_ref=home.at[q, i], dst_ref=relay[q].at[pl.ds(nt * z, nt)],
            send_sem=s4.at[q], recv_sem=r4.at[q], device_id={"ta": relay_at(i)}, device_id_type=MESH)

    def final_copy(q, there):
        return pltpu.make_async_remote_copy(
            src_ref=post.at[q, there], dst_ref=back.at[q, my_relay],
            send_sem=s5.at[q], recv_sem=r5.at[q], device_id={"ta": there}, device_id_type=MESH)

    def reduce_chunk(q):
        with jax.named_scope("reduced%d" % q):
            @pl.when(sender == c)
            def _():
                settle(parts.at[q, pl.ds(0, nx - 1)], r3.at[q])

            @pl.when(sender != c)
            def _():
                settle(parts.at[q], r3.at[q])

        for tl in range(nt):
            for reim in range(2):
                total = parts[q, 0, tl, reim]
                for xs in range(1, nx):
                    total += parts[q, xs, tl, reim]
                for i in range(per):
                    home[q, reim * per + i, tl] = total[i * piece:(i + 1) * piece, :]

        for i in range(relays):
            @pl.when(relay_at(i) != z)
            def _():
                return_copy(q, i).start()

            @pl.when(relay_at(i) == z)
            def _():
                for tl in range(nt):
                    relay[q][nt * z + tl] = home[q, i, tl]

    def relay_chunk(q):
        @pl.when(my_relay < relays)
        def _():
            with jax.named_scope("relayed%d" % q):
                settle(relay[q].at[pl.ds(0, nt * (nz - 1))], r4.at[q])

            for there in range(nz):
                for tl in range(nt):
                    post[q, there, tl] = relay[q][order[nt * there + tl]]

                @pl.when(there != z)
                def _():
                    final_copy(q, there).start()

            back[q, my_relay] = post[q, z]

    for q in range(Q):
        contract_chunk(q)
    for q in range(Q):
        reduce_chunk(q)
    for q in range(Q):
        relay_chunk(q)

    for q in range(Q):
        settle(mids[q].at[pl.ds(0, nt * (nz - 1))], s1.at[q])
        settle(mail.at[q, pl.ds(0, nz - 1)], s2.at[q])

        @pl.when(sender == c)
        def _():
            settle(part.at[q, pl.ds(0, nx - 1)], s3.at[q])

        @pl.when(sender != c)
        def _():
            settle(part.at[q], s3.at[q])

        @pl.when(my_relay < relays)
        def _():
            settle(home.at[q, pl.ds(0, relays - 1)], s4.at[q])
            settle(post.at[q, pl.ds(0, nz - 1)], s5.at[q])

        @pl.when(my_relay >= relays)
        def _():
            settle(home.at[q], s4.at[q])

    for q in range(Q):
        with jax.named_scope("final%d" % q):
            @pl.when(my_relay < relays)
            def _():
                settle(back.at[q, pl.ds(0, relays - 1)], r5.at[q])

            @pl.when(my_relay >= relays)
            def _():
                settle(back.at[q], r5.at[q])

        with jax.named_scope("asm%d" % q):
            for reim in range(2):
                for i in range(per):
                    for tl in range(nt):
                        got = back[q, reim * per + i, tl]
                        for j in range(piece // keep):
                            at = (i * (piece // keep) + j) * Q * keep + q * keep
                            flat[tl, reim, at:at + keep, :] = got[j * keep:(j + 1) * keep, :]

    with jax.named_scope("outs"):
        for s in range(spin):
            out_ref[:, :, s] = flat[:, :, :, s * ns:(s + 1) * ns]


def solution(mesh):
    nz, nx, nc = mesh.shape["ta"], mesh.shape["xyz"], mesh.shape["src"]

    def local(spinors, eigvecs, group_of, source_ids):
        ns, nt, _, spin, colours, sites = spinors.shape
        kk = eigvecs.shape[1]
        blocks = sites // LANES
        depth = 2 * colours * blocks
        keep = kk // (nc * nz * Q)
        rows = ns * spin
        ks = nz * keep
        spin_view = spinors.transpose(0, 1, 2, 4, 3, 5).reshape(ns, nt, 2, colours, spin, blocks, LANES)
        spin_view = spin_view.transpose(0, 1, 2, 3, 5, 4, 6).reshape(ns, nt, depth * spin, LANES)
        vec_view = eigvecs.transpose(0, 1, 3, 2, 4).reshape(nt, kk, colours, 2, blocks, LANES)
        vec_view = vec_view.transpose(0, 1, 2, 4, 3, 5).reshape(nt, kk * depth, LANES)
        step = ks * nc // nx
        relays = RELAYS
        sizes = (nz, nx, nc, ns, nt, spin, depth, keep, relays)
        f32, bf16 = jnp.float32, jnp.bfloat16
        dma = pltpu.SemaphoreType.DMA
        small = (step * 2 // relays, LANES)
        out = pl.pallas_call(
            functools.partial(kernel, sizes),
            out_shape=jax.ShapeDtypeStruct((nt, 2, spin, kk // nx, ns), f32),
            in_specs=[pl.BlockSpec(memory_space=pl.ANY)] * 4,
            out_specs=pl.BlockSpec(memory_space=pltpu.VMEM),
            scratch_shapes=[
                pltpu.SMEM((nz * nt,), jnp.int32),
                pltpu.SMEM((ns,), jnp.int32),
                pltpu.SMEM((nz * nt,), jnp.int32),
                pltpu.SMEM((nz * nt,), jnp.int32),
                pltpu.SMEM((ns,), jnp.int32),
                pltpu.VMEM((ns, nt, depth * spin, LANES), f32),
                pltpu.VMEM((nc, nt, depth, rows, LANES), f32),
                pltpu.VMEM((nt, nc * rows, depth * LANES), bf16),
                pltpu.VMEM((nt, nc * rows, depth * LANES), bf16),
                [pltpu.VMEM((nz * nt, keep * depth, LANES), f32)] * Q,
                pltpu.VMEM((Q, nz, nt, keep * depth, LANES), f32),
                pltpu.VMEM((Q, nt, ks * depth, LANES), f32),
                pltpu.VMEM((4 * ks, depth * LANES), bf16),
                pltpu.VMEM((Q, nx, nt, 2, ks * nc // nx, LANES), f32),
                pltpu.VMEM((Q, nx, nt, 2, ks * nc // nx, LANES), f32),
                pltpu.VMEM((Q, relays, nt) + small, f32),
                [pltpu.VMEM((nz * nt,) + small, f32)] * Q,
                pltpu.VMEM((Q, nz, nt) + small, f32),
                pltpu.VMEM((Q, relays, nt) + small, f32),
                pltpu.VMEM((nt, 2, kk // nx, rows), f32),
                pltpu.SemaphoreType.REGULAR((nz,)), pltpu.SemaphoreType.REGULAR((2, nx // 2 - 1)), dma((2,)), dma, dma((Q,)), dma((2,)),
                [dma((Q,))] * 2, [dma((Q,))] * 2, [dma((Q,))] * 2, [dma((Q,))] * 2, [dma((Q,))] * 2,
            ],
            compiler_params=pltpu.CompilerParams(collective_id=0, has_side_effects=True),
        )(group_of, source_ids, vec_view, spin_view)
        return out.transpose(0, 1, 2, 4, 3)

    in_specs = (
        P("src", "ta", None, "job", None, "xyz"),
        P("ta", "job", None, None, "xyz"),
        P(),
        P("src"),
    )
    out_specs = P("ta", None, "job", "src", "xyz")
    return jax.shard_map(local, mesh=mesh, in_specs=in_specs, out_specs=out_specs, check_vma=False)
```

```python
import functools

import jax
import jax.numpy as jnp
from jax import lax
from jax.experimental import pallas as pl
from jax.experimental.pallas import tpu as pltpu
from jax.sharding import PartitionSpec as P

MESH = pl.DeviceIdType.MESH
LANES = 128
Q = 2
EARLY = 8
LATE = 0
RELAYS = 4
BEFORE = 3


def kernel(sizes, group_hbm, ids_hbm, vec_ref, spin_ref, out_ref,
           group_ref, ids_ref, rank, order, inverse, raw, both, high, low, mids, mail, gathered, left,
           part, parts, home, relay, post, back, flat,
           above, along, small_sem, load_sem, own_sem, pair_sem, *pairs):
    (s1, r1), (s2, r2), (s3, r3), (s4, r4), (s5, r5) = pairs
    nz, nx, nc, ns, nt, spin, depth, keep, relays = sizes
    z, x, c = lax.axis_index("ta"), lax.axis_index("xyz"), lax.axis_index("src")
    other = 1 - c
    rows = ns * spin
    chunk = keep * depth
    half = nx // nc

    def far(d):
        return lax.rem(z + d, nz)

    def settle(ref, sem):
        pltpu.make_async_copy(ref, ref, sem).wait()

    place = lax.rem(z + nz - 1, nz)

    def at_place(p):
        return lax.rem(p + 1, nz)

    barrier = pltpu.get_barrier_semaphore()

    @pl.loop(0, nz - 1 - place)
    def _(i):
        pl.semaphore_signal(barrier, inc=1, device_id={"ta": at_place(nz - 1 - i)}, device_id_type=MESH)

    right, left_x = lax.rem(x + 1, nx), lax.rem(x + nx - 1, nx)
    for there in (right, left_x):
        pl.semaphore_signal(barrier, inc=1, device_id={"xyz": there}, device_id_type=MESH)
    pl.semaphore_signal(barrier, inc=1, device_id={"src": other}, device_id_type=MESH)

    loads = [
        pltpu.make_async_copy(group_hbm, group_ref, small_sem.at[0]),
        pltpu.make_async_copy(ids_hbm, ids_ref, small_sem.at[1]),
        pltpu.make_async_copy(spin_ref, raw, load_sem),
    ]
    for load in loads:
        load.start()
    pl.semaphore_wait(barrier, 3 + place)

    def share(q, there):
        first = (c * (nz * Q * keep) + there * (Q * keep) + q * keep) * depth
        return vec_ref.at[:, pl.ds(pl.multiple_of(first, 8), chunk), :]

    def spread(q, d):
        return pltpu.make_async_remote_copy(
            src_ref=share(q, far(d)), dst_ref=mids[q].at[pl.ds(nt * z, nt)],
            send_sem=s1.at[q], recv_sem=r1.at[q], device_id={"ta": far(d)}, device_id_type=MESH)

    def deliver(q, d):
        return pltpu.make_async_remote_copy(
            src_ref=mail.at[q, d], dst_ref=gathered.at[q, :, pl.ds(pl.multiple_of(z * chunk, 8), chunk), :],
            send_sem=s2.at[q], recv_sem=r2.at[q], device_id={"ta": far(d)}, device_id_type=MESH)

    outward = sorted(range(1, nz), key=lambda d: -min(d, nz - d))
    with jax.named_scope("known"):
      for d in outward:
        @pl.when(d >= nz - place)
        def _():
            pl.semaphore_signal(above.at[place], inc=1, device_id={"ta": far(d)}, device_id_type=MESH)

    for q in range(Q):
        for d in outward:
            @pl.when(d >= nz - place)
            def _():
                spread(q, d).start()

        pltpu.make_async_copy(share(q, z), mids[q].at[pl.ds(nt * z, nt)], own_sem.at[q]).start()

    count = nz * nt

    def prepare():
        hops = list(range(nx // 2 - 1))

        def tell(j):
            pl.semaphore_signal(along.at[0, j], inc=1, device_id={"xyz": left_x}, device_id_type=MESH)
            pl.semaphore_signal(along.at[1, j], inc=1, device_id={"xyz": right}, device_id_type=MESH)

        def hear(j):
            pl.semaphore_wait(along.at[0, j], 1)
            pl.semaphore_wait(along.at[1, j], 1)

        tell(hops[0])
        loads[0].wait()
        loads[1].wait()


        @pl.loop(0, count)
        def _(t):
            mine = group_ref[t] * count + t
            total = jnp.int32(0)
            for u in range(count):
                total += jnp.where(group_ref[u] * count + u < mine, 1, 0)
            rank[t] = total

        @pl.loop(0, count)
        def _(r):
            total = jnp.int32(0)
            for u in range(count):
                total = jnp.maximum(total, jnp.where(rank[u] == r, u, 0))
            order[r] = total

        @pl.loop(0, ns)
        def _(j):
            total = jnp.int32(0)
            for u in range(ns):
                total = jnp.maximum(total, jnp.where(ids_ref[u] - c * ns == j, u, 0))
            inverse[j] = total

        for j in hops[:-1]:
            hear(j)
            tell(j + 1)
        loads[2].wait()

        @pl.loop(0, ns)
        def _(j):
            n = inverse[j]
            for tl in range(nt):
                for g in range(depth):
                    for s in range(spin):
                        both[c, tl, g, pl.ds(s * ns + j, 1), :] = raw[n, tl, g * spin + s:g * spin + s + 1, :]

        pair = pltpu.make_async_remote_copy(
            src_ref=both.at[c], dst_ref=both.at[c], send_sem=pair_sem.at[0], recv_sem=pair_sem.at[1],
            device_id={"src": other}, device_id_type=MESH)
        hear(hops[-1])
        pair.start()
        pair.wait()

        @pl.loop(0, nt)
        def _(tl):
            for core in range(nc):
                for g in range(depth):
                    block = both[core, tl, g]
                    top = block.astype(jnp.bfloat16)
                    high[tl, core * rows:(core + 1) * rows, g * LANES:(g + 1) * LANES] = top
                    low[tl, core * rows:(core + 1) * rows, g * LANES:(g + 1) * LANES] = (block - top.astype(jnp.float32)).astype(jnp.bfloat16)

    with jax.named_scope("early"):
        @pl.when(place < EARLY)
        def _():
            prepare()

    with jax.named_scope("upper"):
        @pl.loop(1, jnp.maximum(LATE - place, 1))
        def _(d):
            pl.semaphore_wait(above.at[place + d], 1)
            for q in range(Q):
                spread(q, d).start()

        @pl.loop(jnp.maximum(LATE - place, 1), nz - place)
        def _(d):
            pl.semaphore_wait(above.at[place + d], 1)
            spread(0, d).start()

        for q in range(1, Q):
            for d in outward:
                @pl.when(jnp.logical_and(place + d >= LATE, place + d < nz))
                def _():
                    spread(q, d).start()

    with jax.named_scope("late"):
        @pl.when(place >= EARLY)
        def _():
            prepare()

    for q in range(Q):
        with jax.named_scope("mid%d" % q):
            settle(mids[q].at[pl.ds(0, nt * (nz - 1))], r1.at[q])

        pltpu.make_async_copy(share(q, z), mids[q].at[pl.ds(nt * z, nt)], own_sem.at[q]).wait()

        @pl.loop(1, nz)
        def _(d):
            for tl in range(nt):
                mail[q, d, tl] = mids[q][rank[nt * far(d) + tl]]

        for tl in range(nt):
            gathered[q, tl, pl.ds(pl.multiple_of(z * chunk, 8), chunk), :] = mids[q][rank[nt * z + tl]]

        for d in outward:
            deliver(q, d).start()

    contract = (((1,), (1,)), ((), ()))
    ks = nz * keep
    colours = depth // 4

    def target(o):
        return lax.rem(x + o, half)

    def reduce_copy(q, o, core, tl):
        xs = target(o)
        return pltpu.make_async_remote_copy(
            src_ref=part.at[q, xs * nc + core, tl], dst_ref=parts.at[q, x, tl],
            send_sem=s3.at[q], recv_sem=r3.at[q],
            device_id={"xyz": half * c + xs, "src": core}, device_id_type=MESH)

    sender = lax.div(x, half)
    step = ks // half
    per = relays // 2
    piece = step // per

    def relay_at(i):
        return lax.rem(i + nz - BEFORE, nz)

    my_relay = lax.rem(z + BEFORE, nz)

    def contract_chunk(q):
        with jax.named_scope("got%d" % q):
            settle(gathered.at[q, :, pl.ds(0, (nz - 1) * chunk)], r2.at[q])

        for tl in range(nt):
            for i in range(colours):
                for b in range(2):
                    re = gathered[q, tl, pl.ds(i * 4 + b * 2, ks, stride=depth), :]
                    im = gathered[q, tl, pl.ds(i * 4 + b * 2 + 1, ks, stride=depth), :]
                    g = i * 2 + b
                    for at, value in ((0, re), (depth // 2, im)):
                        top = value.astype(jnp.bfloat16)
                        rest = (value - top.astype(jnp.float32)).astype(jnp.bfloat16)
                        where = slice((at + g) * LANES, (at + g + 1) * LANES)
                        cross = slice((depth // 2 - at + g) * LANES, (depth // 2 - at + g + 1) * LANES)
                        left[0:ks, where] = top
                        left[2 * ks:3 * ks, where] = rest
                        left[ks:2 * ks, cross] = top if at == 0 else -top
                        left[3 * ks:4 * ks, cross] = rest if at == 0 else -rest
            one = lax.dot_general(left[...], high[tl], contract, preferred_element_type=jnp.float32)
            two = lax.dot_general(left[0:2 * ks, :], low[tl], contract, preferred_element_type=jnp.float32)
            total = one[0:2 * ks] + one[2 * ks:4 * ks] + two
            for xs in range(half):
                for core in range(nc):
                    for reim in range(2):
                        part[q, xs * nc + core, tl, reim] = total[reim * ks + xs * step:reim * ks + (xs + 1) * step, core * rows:(core + 1) * rows]

            for o in [0] + sorted(range(1, half), key=lambda o: abs(2 * o - half)):
                for core in range(nc):
                    mine = jnp.logical_and(half * c + target(o) == x, c == core)

                    @pl.when(jnp.logical_not(mine))
                    def _():
                        reduce_copy(q, o, core, tl).start()

                    if o == 0:
                        @pl.when(mine)
                        def _():
                            parts[q, x, tl] = part[q, target(o) * nc + core, tl]

    def return_copy(q, i):
        return pltpu.make_async_remote_copy(
            src_ref=home.at[q, i], dst_ref=relay[q].at[pl.ds(nt * z, nt)],
            send_sem=s4.at[q], recv_sem=r4.at[q], device_id={"ta": relay_at(i)}, device_id_type=MESH)

    def final_copy(q, there):
        return pltpu.make_async_remote_copy(
            src_ref=post.at[q, there], dst_ref=back.at[q, my_relay],
            send_sem=s5.at[q], recv_sem=r5.at[q], device_id={"ta": there}, device_id_type=MESH)

    def reduce_chunk(q):
        with jax.named_scope("reduced%d" % q):
            @pl.when(sender == c)
            def _():
                settle(parts.at[q, pl.ds(0, nx - 1)], r3.at[q])

            @pl.when(sender != c)
            def _():
                settle(parts.at[q], r3.at[q])

        for tl in range(nt):
            for reim in range(2):
                total = parts[q, 0, tl, reim]
                for xs in range(1, nx):
                    total += parts[q, xs, tl, reim]
                for i in range(per):
                    home[q, reim * per + i, tl] = total[i * piece:(i + 1) * piece, :]

        for i in range(relays):
            @pl.when(relay_at(i) != z)
            def _():
                return_copy(q, i).start()

            @pl.when(relay_at(i) == z)
            def _():
                for tl in range(nt):
                    relay[q][nt * z + tl] = home[q, i, tl]

    def relay_chunk(q):
        @pl.when(my_relay < relays)
        def _():
            with jax.named_scope("relayed%d" % q):
                settle(relay[q].at[pl.ds(0, nt * (nz - 1))], r4.at[q])

            for there in range(nz):
                for tl in range(nt):
                    post[q, there, tl] = relay[q][order[nt * there + tl]]

                @pl.when(there != z)
                def _():
                    final_copy(q, there).start()

            back[q, my_relay] = post[q, z]

    for q in range(Q):
        contract_chunk(q)
    for q in range(Q):
        reduce_chunk(q)
    for q in range(Q):
        relay_chunk(q)

    for q in range(Q):
        settle(mids[q].at[pl.ds(0, nt * (nz - 1))], s1.at[q])
        settle(mail.at[q, pl.ds(0, nz - 1)], s2.at[q])

        @pl.when(sender == c)
        def _():
            settle(part.at[q, pl.ds(0, nx - 1)], s3.at[q])

        @pl.when(sender != c)
        def _():
            settle(part.at[q], s3.at[q])

        @pl.when(my_relay < relays)
        def _():
            settle(home.at[q, pl.ds(0, relays - 1)], s4.at[q])
            settle(post.at[q, pl.ds(0, nz - 1)], s5.at[q])

        @pl.when(my_relay >= relays)
        def _():
            settle(home.at[q], s4.at[q])

    for q in range(Q):
        with jax.named_scope("final%d" % q):
            @pl.when(my_relay < relays)
            def _():
                settle(back.at[q, pl.ds(0, relays - 1)], r5.at[q])

            @pl.when(my_relay >= relays)
            def _():
                settle(back.at[q], r5.at[q])

        with jax.named_scope("asm%d" % q):
            for reim in range(2):
                for i in range(per):
                    for tl in range(nt):
                        got = back[q, reim * per + i, tl]
                        for j in range(piece // keep):
                            at = (i * (piece // keep) + j) * Q * keep + q * keep
                            flat[tl, reim, at:at + keep, :] = got[j * keep:(j + 1) * keep, :]

    with jax.named_scope("outs"):
        for s in range(spin):
            out_ref[:, :, s] = flat[:, :, :, s * ns:(s + 1) * ns]


def solution(mesh):
    nz, nx, nc = mesh.shape["ta"], mesh.shape["xyz"], mesh.shape["src"]

    def local(spinors, eigvecs, group_of, source_ids):
        ns, nt, _, spin, colours, sites = spinors.shape
        kk = eigvecs.shape[1]
        blocks = sites // LANES
        depth = 2 * colours * blocks
        keep = kk // (nc * nz * Q)
        rows = ns * spin
        ks = nz * keep
        spin_view = spinors.transpose(0, 1, 2, 4, 3, 5).reshape(ns, nt, 2, colours, spin, blocks, LANES)
        spin_view = spin_view.transpose(0, 1, 2, 3, 5, 4, 6).reshape(ns, nt, depth * spin, LANES)
        vec_view = eigvecs.transpose(0, 1, 3, 2, 4).reshape(nt, kk, colours, 2, blocks, LANES)
        vec_view = vec_view.transpose(0, 1, 2, 4, 3, 5).reshape(nt, kk * depth, LANES)
        step = ks * nc // nx
        relays = RELAYS
        sizes = (nz, nx, nc, ns, nt, spin, depth, keep, relays)
        f32, bf16 = jnp.float32, jnp.bfloat16
        dma = pltpu.SemaphoreType.DMA
        small = (step * 2 // relays, LANES)
        out = pl.pallas_call(
            functools.partial(kernel, sizes),
            out_shape=jax.ShapeDtypeStruct((nt, 2, spin, kk // nx, ns), f32),
            in_specs=[pl.BlockSpec(memory_space=pl.ANY)] * 4,
            out_specs=pl.BlockSpec(memory_space=pltpu.VMEM),
            scratch_shapes=[
                pltpu.SMEM((nz * nt,), jnp.int32),
                pltpu.SMEM((ns,), jnp.int32),
                pltpu.SMEM((nz * nt,), jnp.int32),
                pltpu.SMEM((nz * nt,), jnp.int32),
                pltpu.SMEM((ns,), jnp.int32),
                pltpu.VMEM((ns, nt, depth * spin, LANES), f32),
                pltpu.VMEM((nc, nt, depth, rows, LANES), f32),
                pltpu.VMEM((nt, nc * rows, depth * LANES), bf16),
                pltpu.VMEM((nt, nc * rows, depth * LANES), bf16),
                [pltpu.VMEM((nz * nt, keep * depth, LANES), f32)] * Q,
                pltpu.VMEM((Q, nz, nt, keep * depth, LANES), f32),
                pltpu.VMEM((Q, nt, ks * depth, LANES), f32),
                pltpu.VMEM((4 * ks, depth * LANES), bf16),
                pltpu.VMEM((Q, nx, nt, 2, ks * nc // nx, LANES), f32),
                pltpu.VMEM((Q, nx, nt, 2, ks * nc // nx, LANES), f32),
                pltpu.VMEM((Q, relays, nt) + small, f32),
                [pltpu.VMEM((nz * nt,) + small, f32)] * Q,
                pltpu.VMEM((Q, nz, nt) + small, f32),
                pltpu.VMEM((Q, relays, nt) + small, f32),
                pltpu.VMEM((nt, 2, kk // nx, rows), f32),
                pltpu.SemaphoreType.REGULAR((nz,)), pltpu.SemaphoreType.REGULAR((2, nx // 2 - 1)), dma((2,)), dma, dma((Q,)), dma((2,)),
                [dma((Q,))] * 2, [dma((Q,))] * 2, [dma((Q,))] * 2, [dma((Q,))] * 2, [dma((Q,))] * 2,
            ],
            compiler_params=pltpu.CompilerParams(collective_id=0, has_side_effects=True),
        )(group_of, source_ids, vec_view, spin_view)
        return out.transpose(0, 1, 2, 4, 3)

    in_specs = (
        P("src", "ta", None, "job", None, "xyz"),
        P("ta", "job", None, None, "xyz"),
        P(),
        P("src"),
    )
    out_specs = P("ta", None, "job", "src", "xyz")
    return jax.shard_map(local, mesh=mesh, in_specs=in_specs, out_specs=out_specs, check_vma=False)
```
